128 devices in a mesh: blk: 32 (over x, y_hi, z), span: 4 (over y_lo, core).
Axes of the slice: x: 4, y: 4 (y_hi: 2, y_lo: 2; y = y_hi * 2 + y_lo), z: 4, core: 2. Of those that a mesh axis runs over, the one named last changes fastest.
Arguments:
- fields: float32 [5, 125, 65536], P(None, None, ('blk', 'span')), may hold values from -6 to 6
- section_store: float32 [5, 125, 65536], P(None, None, ('blk', 'span')), may hold values from -6 to 6
- mean_velocity: float32 [3, 125, 65536], P(None, None, ('blk', 'span')), may hold values from -0.6 to 0.6
- sound_speed: float32 [125, 65536], P(None, ('blk', 'span')), may hold values from 0.7 to 1.5
- element_slot: int32 [65536], P(('blk', 'span')), may hold values from 0 to 511, as said below
- face_turn: int32 [32, 16], P('blk', 'span'), may hold values from 0 to 7
- rotor_offset: int32 [16], P('span'), may hold values from 0 to 31
Outputs:
- fields_next: float32 [5, 125, 65536], P(None, None, ('blk', 'span'))
- store_next: float32 [5, 125, 65536], P(None, None, ('blk', 'span'))
The draws below stay inside these ranges and needn't reach their ends.
Inputs may be any that keep to these rules, and one draw needn't show every extreme that they name: `element_slot`: in each aligned block of 512 entries (the elements of one device) every number 0 to 511 appears once.
All inputs are finite; a program needn't handle non-finite values.
Results may differ from the reference program's by a relative error of at most 0.0003.
Values sent between devices are 32-bit elements; how exact they have to be, the bound alone decides.
A program may use at most 128 MiB of HBM per device.

```python
import jax
import jax.numpy as jnp
import numpy as np
from jax import lax

ORDER = 4
ET = 1
ES = 4
EA = 128
ELEM_DEV = 512
NT = 32
NS = 16
ELEMS = 65536
N_BLK = 32
N_SPAN = 4


def draw_element_slot(key, part):
    block_keys = jax.random.split(jax.random.fold_in(key, 17), ELEMS // ELEM_DEV)

    def block_order(block_key):
        return jax.random.permutation(block_key, ELEM_DEV)
    orders = jax.vmap(block_order)(block_keys)
    return orders.reshape(ELEMS).astype(jnp.int32)


def draw_rotor_offset(key, part):
    row_keys = jax.random.split(jax.random.fold_in(key, 29), 5)
    base = jax.random.randint(row_keys[0], (NS,), 0, NT)
    far_row = N_BLK // 2 * ET + jax.random.randint(row_keys[1], (), 0, ET)
    near_row = jax.random.randint(row_keys[2], (), 1, ET + 1)
    full_row = (N_BLK - 1) * ET + jax.random.randint(row_keys[3], (), 0, ET)
    base = base.at[0].set(far_row).at[1].set(near_row).at[2].set(full_row)
    order = jax.random.permutation(row_keys[4], NS)
    return base[order].astype(jnp.int32)


def touch_ends(drawn, stream_key, low, top_value):
    spot = [jax.random.randint(jax.random.fold_in(stream_key, axis), (), 0, length) for axis, length in enumerate(drawn.shape)]
    main_axis = drawn.shape.index(max(drawn.shape))
    next_to = spot[:main_axis] + [(spot[main_axis] + 1) % drawn.shape[main_axis]] + spot[main_axis + 1:]
    return drawn.at[tuple(spot)].set(low).at[tuple(next_to)].set(top_value)


def shard_levels(key, extent, cuts, least, top_value):
    level, own = 1.0, jax.random.fold_in(key, 6)
    for position, blocks in cuts:
        steps = jnp.exp(jax.random.uniform(jax.random.fold_in(own, position), (blocks,), jnp.float32, least / len(cuts), top_value / len(cuts)))
        level = level * jnp.repeat(steps, extent[position] // blocks).reshape([-1 if axis == position else 1 for axis in range(len(extent))])
    return level


def scatter_about(own_key, dims, spread, most, cuts=(), kind=jnp.bfloat16):
    level = shard_levels(own_key, dims, cuts, -0.22, 0.18) if cuts else 1.0
    drawn = jax.random.normal(own_key, dims, jnp.float32) * spread * level
    return jnp.minimum(jnp.maximum(drawn, -most), most).astype(kind)


def setup_inputs(seed: int = 0) -> dict:
    streams_of = jax.random.split(jax.random.key(seed), 8)
    fields = scatter_about(streams_of[0], (5, (ORDER + 1) ** 3, ELEMS), 1.0, 6.0, ((2, 128),), jnp.float32)
    section_store = scatter_about(streams_of[1], (5, (ORDER + 1) ** 3, ELEMS), 1.0, 6.0, ((2, 128),), jnp.float32)
    mean_velocity = jnp.clip(jax.random.uniform(streams_of[2], (3, (ORDER + 1) ** 3, ELEMS), jnp.float32, -0.6, 0.6) * shard_levels(streams_of[2], (3, (ORDER + 1) ** 3, ELEMS), ((2, 128),), -0.4, 0.0), -0.6, 0.6)
    sound_speed = jnp.clip(0.7 + 0.8 * jax.random.uniform(streams_of[3], ((ORDER + 1) ** 3, ELEMS), jnp.float32) ** shard_levels(streams_of[3], ((ORDER + 1) ** 3, ELEMS), ((1, 128),), -0.2, 0.2), 0.7, 1.5)
    element_slot = draw_element_slot(jax.random.fold_in(streams_of[7], 71), 0)
    face_turn = touch_ends(jax.random.randint(streams_of[5], (NT, NS), 0, 8), jax.random.fold_in(streams_of[5], 1), 0, 7).astype(jnp.int32)
    rotor_offset = draw_rotor_offset(jax.random.fold_in(streams_of[7], 71), 0)
    return dict(fields=fields, section_store=section_store, mean_velocity=mean_velocity, sound_speed=sound_speed, element_slot=element_slot, face_turn=face_turn, rotor_offset=rotor_offset)


section_decay = -567301805773.0 / 1357537059087.0
section_gain = 5161836677717.0 / 13612068292357.0
time_step = 0.05
metric_scale = (1.0, 1.5, 0.75)
end_weight = 0.1

def lobatto_slopes():
    inner_root = np.sqrt(3.0 / 7.0)
    points = np.array([-1.0, -inner_root, 0.0, inner_root, 1.0])
    node_count = points.shape[0]
    slope_values = np.zeros((node_count, node_count))
    for row_index in range(node_count):
        for column_index in range(node_count):
            if row_index == column_index:
                slope_values[row_index, column_index] = sum((1.0 / (points[row_index] - points[other_index]) for other_index in range(node_count) if other_index != row_index))
            else:
                product_row = np.prod([points[row_index] - points[other_index] for other_index in range(node_count) if other_index != row_index])
                product_column = np.prod([points[column_index] - points[other_index] for other_index in range(node_count) if other_index != column_index])
                slope_values[row_index, column_index] = product_row / (product_column * (points[row_index] - points[column_index]))
    return slope_values

def face_of(element_data, direction, which_end):
    return lax.index_in_dim(element_data, which_end, axis=1 + direction, keepdims=False)

def normal_trace(face_data, direction):
    return jnp.concatenate([face_data[:5], face_data[5 + direction:6 + direction], face_data[8:9]], axis=0)

def normal_flux(face_data, direction):
    state_part = face_data[:5]
    flow_speed = face_data[5]
    sound_part = face_data[6]
    normal_velocity = state_part[1 + direction]
    pressure = state_part[4]
    zero_part = jnp.zeros_like(pressure)
    coupled = jnp.stack([normal_velocity] + [pressure if axis_index == direction else zero_part for axis_index in range(3)] + [normal_velocity])
    return flow_speed[None] * state_part + sound_part[None] * coupled

def face_flux(left_side, right_side, direction):
    wave_reach = jnp.maximum(jnp.abs(left_side[5]) + left_side[6], jnp.abs(right_side[5]) + right_side[6])
    return 0.5 * (normal_flux(left_side, direction) + normal_flux(right_side, direction)) - 0.5 * wave_reach[None] * (right_side[:5] - left_side[:5])

def wall_ghost(face_data):
    flip_sign = jnp.array([1.0, 1.0, -1.0, 1.0, 1.0, 1.0, 1.0], jnp.float32).reshape((7,) + (1,) * (face_data.ndim - 1))
    return face_data * flip_sign

def turn_face(face_data, turn_codes, inverse):
    result = jnp.zeros_like(face_data)
    for turn_code in range(8):
        turned = face_data
        if inverse:
            if turn_code & 2:
                turned = jnp.flip(turned, 2)
            if turn_code & 1:
                turned = jnp.flip(turned, 1)
            if turn_code & 4:
                turned = jnp.swapaxes(turned, 1, 2)
        else:
            if turn_code & 4:
                turned = jnp.swapaxes(turned, 1, 2)
            if turn_code & 1:
                turned = jnp.flip(turned, 1)
            if turn_code & 2:
                turned = jnp.flip(turned, 2)
        result = result + jnp.where(turn_codes == turn_code, turned, 0.0)
    return result

def pick_cells(cycle_data, cell_index):
    full_index = jnp.broadcast_to(cell_index[None, None, None], cycle_data.shape[:3] + cell_index.shape)
    return jnp.take_along_axis(cycle_data, full_index, axis=3)

def surface_terms(segment, direction, ghost_low, ghost_high):
    plus_side = normal_trace(face_of(segment, direction, 4), direction)
    minus_side = normal_trace(face_of(segment, direction, 0), direction)
    element_axis = 3 + direction
    left_side = jnp.concatenate([ghost_low, plus_side], axis=element_axis)
    right_side = jnp.concatenate([minus_side, ghost_high], axis=element_axis)
    fluxes = face_flux(left_side, right_side, direction)
    face_total = fluxes.shape[element_axis]
    upper_part = normal_flux(plus_side, direction) - lax.slice_in_dim(fluxes, 1, face_total, axis=element_axis)
    lower_part = lax.slice_in_dim(fluxes, 0, face_total - 1, axis=element_axis) - normal_flux(minus_side, direction)
    mark_shape = [1] * 7
    mark_shape[1 + direction] = 5
    high_mark = (jnp.arange(5) == 4).astype(jnp.float32).reshape(mark_shape)
    low_mark = (jnp.arange(5) == 0).astype(jnp.float32).reshape(mark_shape)
    weight = metric_scale[direction] / end_weight
    return weight * (jnp.expand_dims(upper_part, 1 + direction) * high_mark + jnp.expand_dims(lower_part, 1 + direction) * low_mark)

def volume_terms(element_data):
    slope_table = jnp.asarray(lobatto_slopes(), jnp.float32)
    einsum_forms = ('ni,fijkxyz->fnjkxyz', 'nj,fijkxyz->finkxyz', 'nk,fijkxyz->fijnxyz')
    summed = jnp.zeros((5,) + element_data.shape[1:], jnp.float32)
    for direction in range(3):
        volume_flux = normal_flux(normal_trace(element_data, direction), direction)
        summed = summed - metric_scale[direction] * jnp.einsum(einsum_forms[direction], slope_table, volume_flux, precision=lax.Precision.HIGHEST)
    return summed

def block_rates(element_data, theta_low, theta_high, span_low, span_high, from_rotor, from_stator):
    half_axial = element_data.shape[6] // 2
    rates = volume_terms(element_data)
    rates = rates + surface_terms(element_data, 0, theta_low, theta_high)
    rates = rates + surface_terms(element_data, 1, span_low, span_high)
    stator = element_data[..., :half_axial]
    rotor = element_data[..., half_axial:]
    inlet_trace = normal_trace(face_of(stator, 2, 0)[..., 0:1], 2)
    inlet = jnp.concatenate([jnp.zeros_like(inlet_trace[:5]), inlet_trace[5:]], axis=0)
    outlet_trace = normal_trace(face_of(rotor, 2, 4)[..., half_axial - 1:half_axial], 2)
    outlet = jnp.concatenate([jnp.zeros_like(outlet_trace[:5]), outlet_trace[5:]], axis=0)
    axial_terms = jnp.concatenate([surface_terms(stator, 2, inlet, from_rotor), surface_terms(rotor, 2, from_stator, outlet)], axis=6)
    return rates + axial_terms

def reference(fields, section_store, mean_velocity, sound_speed, element_slot, face_turn, rotor_offset):
    node_count = ORDER + 1
    block_count = N_BLK * N_SPAN
    half_axial = EA // 2
    cycle_size = ET * N_BLK
    block_turns = face_turn.reshape(N_BLK, ET, N_SPAN, ES)

    def block_data(block_index):
        start = block_index * ELEM_DEV
        slots = lax.dynamic_slice_in_dim(element_slot, start, ELEM_DEV, 0)
        local_fields = lax.dynamic_slice_in_dim(fields, start, ELEM_DEV, 2)
        local_velocity = lax.dynamic_slice_in_dim(mean_velocity, start, ELEM_DEV, 2)
        local_sound = lax.dynamic_slice_in_dim(sound_speed, start, ELEM_DEV, 1)
        stacked = jnp.concatenate([local_fields, local_velocity, local_sound[None]], axis=0)
        element_data = jnp.take(stacked, slots, axis=2).reshape(9, node_count, node_count, node_count, ET, ES, EA)
        return (slots, element_data)

    def codes_of(block_index):
        return block_turns[block_index // N_SPAN, :, block_index % N_SPAN, :]

    def trace_pass(block_index):
        slots, element_data = block_data(block_index)
        theta_pair = jnp.concatenate([face_of(element_data, 0, 0)[:, :, :, 0:1], face_of(element_data, 0, 4)[:, :, :, ET - 1:ET]], axis=3)
        span_pair = jnp.concatenate([face_of(element_data, 1, 0)[:, :, :, :, 0:1], face_of(element_data, 1, 4)[:, :, :, :, ES - 1:ES]], axis=4)
        stator_face = face_of(element_data, 2, 4)[..., half_axial - 1]
        rotor_face = turn_face(face_of(element_data, 2, 0)[..., half_axial], codes_of(block_index), True)
        return (theta_pair, span_pair, stator_face, rotor_face)
    block_ids = jnp.arange(block_count, dtype=jnp.int32)
    theta_pairs, span_pairs, stator_faces, rotor_faces = lax.map(trace_pass, block_ids)

    def rate_pass(block_index):
        slots, element_data = block_data(block_index)
        sector = block_index // N_SPAN
        slab_index = block_index % N_SPAN
        before = (sector - 1) % N_BLK * N_SPAN + slab_index
        after = (sector + 1) % N_BLK * N_SPAN + slab_index
        theta_low = normal_trace(theta_pairs[before][:, :, :, 1:2], 0)
        theta_high = normal_trace(theta_pairs[after][:, :, :, 0:1], 0)
        own_span = span_pairs[block_index]
        below = normal_trace(span_pairs[jnp.maximum(block_index - 1, 0)][:, :, :, :, 1:2], 1)
        above = normal_trace(span_pairs[jnp.minimum(block_index + 1, block_count - 1)][:, :, :, :, 0:1], 1)
        hub = wall_ghost(normal_trace(own_span[:, :, :, :, 0:1], 1))
        casing = wall_ghost(normal_trace(own_span[:, :, :, :, 1:2], 1))
        span_low = jnp.where(slab_index > 0, below, hub)
        span_high = jnp.where(slab_index < N_SPAN - 1, above, casing)
        cycle_blocks = jnp.arange(N_BLK, dtype=jnp.int32) * N_SPAN + slab_index
        stator_cycle = jnp.moveaxis(stator_faces[cycle_blocks], 0, 3).reshape(9, node_count, node_count, cycle_size, ES)
        rotor_cycle = jnp.moveaxis(rotor_faces[cycle_blocks], 0, 3).reshape(9, node_count, node_count, cycle_size, ES)
        cycle_cells = sector * ET + jnp.arange(ET, dtype=jnp.int32)
        offsets = lax.dynamic_slice_in_dim(rotor_offset, (slab_index * ES).astype(jnp.int32), ES, 0)
        stator_near = pick_cells(stator_cycle, (cycle_cells[:, None] - offsets[None, :]) % cycle_size)
        rotor_near = pick_cells(rotor_cycle, (cycle_cells[:, None] + offsets[None, :]) % cycle_size)
        from_stator = normal_trace(turn_face(stator_near, codes_of(block_index), False), 2)[..., None]
        from_rotor = normal_trace(rotor_near, 2)[..., None]
        rates = block_rates(element_data, theta_low, theta_high, span_low, span_high, from_rotor, from_stator)
        stored = jnp.zeros((5, node_count ** 3, ELEM_DEV), jnp.float32).at[:, :, slots].set(rates.reshape(5, node_count ** 3, ELEM_DEV))
        start = block_index * ELEM_DEV
        old_store = lax.dynamic_slice_in_dim(section_store, start, ELEM_DEV, 2)
        old_fields = lax.dynamic_slice_in_dim(fields, start, ELEM_DEV, 2)
        new_store = section_decay * old_store + time_step * stored
        new_fields = old_fields + section_gain * new_store
        return (new_fields, new_store)
    fields_blocks, store_blocks = lax.map(rate_pass, block_ids)
    fields_next = jnp.moveaxis(fields_blocks, 0, 2).reshape(5, node_count ** 3, ELEMS)
    store_next = jnp.moveaxis(store_blocks, 0, 2).reshape(5, node_count ** 3, ELEMS)
    return (fields_next, store_next)
```

```python
import functools

import jax
import jax.numpy as jnp
import numpy as np
from jax import lax
from jax.experimental import pallas as pl
from jax.experimental.pallas import tpu as pltpu
from jax.sharding import PartitionSpec as P

MESH = pl.DeviceIdType.MESH
F32, BF16, I32 = jnp.float32, jnp.bfloat16, jnp.int32

section_decay = -567301805773.0 / 1357537059087.0
section_gain = 5161836677717.0 / 13612068292357.0
time_step = 0.05
metric_scale = (1.0, 1.5, 0.75)
end_weight = 0.1

NB = 512
HALF = 64
RADICES = (4, 2, 4)
CHUNKS = ((0, 48), (48, 48), (96, 48), (144, 32))
PACK_ROWS = 176


def lobatto_slopes():
    root = np.sqrt(3.0 / 7.0)
    x = np.array([-1.0, -root, 0.0, root, 1.0])
    table = np.zeros((5, 5))
    for r in range(5):
        for c in range(5):
            others = [o for o in range(5) if o != r]
            if r == c:
                table[r, c] = sum(1.0 / (x[r] - x[o]) for o in others)
            else:
                top = np.prod([x[r] - x[o] for o in others])
                low = np.prod([x[c] - x[o] for o in range(5) if o != c])
                table[r, c] = top / (low * (x[r] - x[c]))
    return table


def slope_matrices():
    d, e = lobatto_slopes(), np.eye(5)
    full = [np.kron(np.kron(d, e), e), np.kron(np.kron(e, d), e), np.kron(np.kron(e, e), d)]
    return np.stack([-g * m for g, m in zip(metric_scale, full)]).astype(np.float32)


def halves(x):
    high = x.astype(BF16)
    return high, (x - high.astype(F32)).astype(BF16)


def moved(x, table, transposed=False):
    rows = x.shape[0]
    high, low = halves(x)
    both = jnp.concatenate([high, low], axis=0)
    dims = (((1,), (1 if transposed else 0,)), ((), ()))
    out = lax.dot_general(both, table, dims, preferred_element_type=F32)
    return out[:rows] + out[rows:]


def flux(q, m, c, d):
    out = [m * v for v in q]
    out[0] = out[0] + c * q[1 + d]
    out[1 + d] = out[1 + d] + c * q[4]
    out[4] = out[4] + c * q[1 + d]
    return out


def face_parts(left, right, d):
    ql, ml, cl = left[:5], left[5], left[6]
    qr, mr, cr = right[:5], right[5], right[6]
    reach = jnp.maximum(jnp.abs(ml) + cl, jnp.abs(mr) + cr)
    fl, fr = flux(ql, ml, cl, d), flux(qr, mr, cr, d)
    return [a - b for a, b in zip(fl, fr)], [reach * (b - a) for a, b in zip(ql, qr)]


def one_hot(row, count):
    k = lax.broadcasted_iota(I32, (count, row.shape[1]), 0).astype(F32)
    return jnp.where(k == row, 1.0, 0.0).astype(BF16)


def turned(x, code, inverse):
    lane = lax.broadcasted_iota(I32, (8, 128), 1)
    n = lane & 31
    i = (n * 13) >> 6
    k = n - i * 5
    ok = n < 25
    base = lane - n

    def apply(v, bit, target):
        index = jnp.where(ok, base + target, lane)
        return jnp.where((code & bit) != 0, jnp.take_along_axis(v, index, axis=1), v)

    swap, first, second = (4, k * 5 + i), (1, (4 - i) * 5 + k), (2, i * 5 + 4 - k)
    for bit, target in (second, first, swap) if inverse else (swap, first, second):
        x = apply(x, bit, target)
    return x


def kernel(
    radices,
    nblk,
    nspan,
    fields,
    mean,
    sound,
    slot_hbm,
    slopes_hbm,
    turn,
    offset,
    rates,
    x,
    acc,
    slot,
    slopes,
    table,
    pack,
    recv,
    near,
    face,
    grid,
    corr,
    sp_send,
    sp_recv,
    stage,
    hops,
    load_sem,
    circ_send,
    circ_recv,
    span_send,
    span_recv,
    hop_send,
    hop_recv,
):
    t = lax.axis_index("blk")
    slab = lax.axis_index("span")
    after, before = lax.rem(t + 1, nblk), lax.rem(t + nblk - 1, nblk)
    above, below = lax.rem(slab + 1, nspan), lax.rem(slab + nspan - 1, nspan)

    digits, weights, rest, weight = [], [], t, 1
    for radix in radices:
        digits.append(lax.rem(rest, radix))
        weights.append(weight)
        rest = rest // radix
        weight *= radix
    peers = []
    for pos, radix in enumerate(radices):
        for step in range(1, radix):
            to = t + (lax.rem(digits[pos] + step, radix) - digits[pos]) * weights[pos]
            peers.append((pos, step, to))

    barrier = pltpu.get_barrier_semaphore()
    for to in (after, before):
        pl.semaphore_signal(barrier, inc=1, device_id={"blk": to}, device_id_type=MESH)
    for to in (above, below):
        pl.semaphore_signal(barrier, inc=1, device_id={"span": to}, device_id_type=MESH)
    for _, _, to in peers:
        pl.semaphore_signal(barrier, inc=1, device_id={"blk": to}, device_id_type=MESH)

    def load(src):
        if src < 5:
            array = fields.at[src]
        else:
            array = mean.at[src - 5] if src < 8 else sound
        return [
            pltpu.make_async_copy(array.at[:, pl.ds(128 * b, 128)], x.at[src, b], load_sem.at[src, b])
            for b in range(4)
        ]

    def cells(src, rows=slice(0, 125)):
        return jnp.concatenate([x[src, b, rows, :] for b in range(4)], axis=1)

    load_slot = pltpu.make_async_copy(slot_hbm, slot, load_sem.at[9, 0])
    load_slopes = pltpu.make_async_copy(slopes_hbm, slopes, load_sem.at[9, 1])
    load_slot.start()
    for src in (0, 1, 2, 3, 4, 5, 8, 6, 7):
        for copy in load(src):
            copy.start()
    load_slopes.start()

    load_slot.wait()
    slot_row = slot[...].astype(F32)
    table[...] = one_hot(slot_row, NB)
    for end in range(2):
        pack[end, 0:1, :] = slot_row

    for at, src in enumerate((0, 1, 2, 3, 4, 5, 8)):
        for copy in load(src):
            copy.wait()
        for end in range(2):
            pack[end, 1 + 25 * at : 26 + 25 * at, :] = cells(src, slice(100 * end, 100 * end + 25))

    pl.semaphore_wait(barrier, 4 + len(peers))

    def circ(end, part):
        start, rows = CHUNKS[part]
        return pltpu.make_async_remote_copy(
            src_ref=pack.at[end, pl.ds(start, rows), :],
            dst_ref=recv.at[1 - end, pl.ds(start, rows), :],
            send_sem=circ_send.at[end, part],
            recv_sem=circ_recv.at[1 - end, part],
            device_id={"blk": after if end == 1 else before},
            device_id_type=MESH,
        )

    for end in range(2):
        circ(end, 0).start()

    for src in (6, 7):
        for copy in load(src):
            copy.wait()
    for d in (2, 1):
        for at, src in enumerate((0, 1, 2, 3, 4, 4 + 1 + d, 8)):
            for end in range(2):
                kind = 2 * (d - 1) + end
                if d == 2:
                    face[kind, 32 * at : 32 * at + 25, :] = cells(src, pl.ds(4 * end, 25, stride=5))
                else:
                    for i in range(5):
                        rows = slice(25 * i + 20 * end, 25 * i + 20 * end + 5)
                        face[kind, 32 * at + 5 * i : 32 * at + 5 * i + 5, :] = cells(src, rows)

    lane = lax.broadcasted_iota(I32, (8, NB), 1)
    sub = lax.broadcasted_iota(I32, (8, NB), 0)
    wanted = jnp.where(sub < 4, sub * 128 + (HALF - 1), (sub - 4) * 128 + HALF)
    column = jnp.sum(jnp.where(lane == wanted, slot_row, 0.0), axis=1, keepdims=True)
    hot = jnp.where(lane.astype(F32) == column, 1.0, 0.0)
    dims = (((1,), (1,)), ((), ()))
    packet = jnp.zeros((8, 256), F32)
    for kind, rows in ((3, sub < 4), (2, sub >= 4)):
        pick = jnp.where(rows, hot, 0.0).astype(BF16)
        for part in halves(face[kind]):
            packet = packet + lax.dot_general(pick, part, dims, preferred_element_type=F32)

    sub1 = lax.broadcasted_iota(I32, (8, 128), 0)
    row = sub1 & 3
    is_stator = sub1 < 4

    def per_row(values):
        out = jnp.full((8, 128), values[3], I32)
        for s in range(3):
            out = jnp.where(row == s, values[s], out)
        return out

    code = per_row([turn[0, s] for s in range(4)])
    shift = per_row([offset[s] for s in range(4)])
    shift = jnp.where(is_stator, shift, (nblk - shift) & (nblk - 1))
    pair = [packet[:, :128], packet[:, 128:]]
    pair = [jnp.where(is_stator, p, turned(p, code, True)) for p in pair]

    def hop(number):
        pos, step, to = peers[number]
        return pltpu.make_async_remote_copy(
            src_ref=stage.at[pos],
            dst_ref=hops.at[number],
            send_sem=hop_send.at[number],
            recv_sem=hop_recv.at[number],
            device_id={"blk": to},
            device_id_type=MESH,
        )

    def start_hops(pos, pair):
        for h in range(2):
            stage[pos, :, 128 * h : 128 * h + 128] = pair[h]
        for number, (p, _, _) in enumerate(peers):
            if p == pos:
                hop(number).start()

    start_hops(0, pair)
    for part in range(1, len(CHUNKS)):
        for end in range(2):
            circ(end, part).start()

    for kind in (1, 0):
        grid[kind] = moved(face[kind], table[...])
        sp_send[kind] = grid[kind, 0:224, 384 * kind : 384 * kind + 128]

    def span(end):
        return pltpu.make_async_remote_copy(
            src_ref=sp_send.at[end],
            dst_ref=sp_recv.at[1 - end],
            send_sem=span_send.at[end],
            recv_sem=span_recv.at[1 - end],
            device_id={"span": above if end == 1 else below},
            device_id_type=MESH,
        )

    for end in range(2):
        span(end).start()
    for kind in (2, 3):
        grid[kind] = moved(face[kind], table[...])

    carry = jnp.zeros((8, 128), I32)

    def take_hops(pos, pair, carry):
        radix = radices[pos]
        digit = lax.rem(shift // weights[pos], radix) + carry
        source = lax.rem(digits[pos] + 2 * radix - digit, radix)
        next_carry = (source + digit - digits[pos]) // radix
        distance = lax.rem(digit, radix)
        for number, (p, step, _) in enumerate(peers):
            if p == pos:
                hop(number).wait()
                for h in range(2):
                    arrived = hops[number, :, 128 * h : 128 * h + 128]
                    pair[h] = jnp.where(distance == step, arrived, pair[h])
        return pair, next_carry

    load_slopes.wait()
    velocity = (5, 6, 7)

    def volume(f):
        total = None
        for d in range(3):
            fx = cells(velocity[d]) * cells(f)
            if f == 0 or f == 4:
                fx = fx + cells(8) * cells(1 + d)
            elif f == 1 + d:
                fx = fx + cells(8) * cells(4)
            part = jnp.dot(slopes[d], fx, precision=lax.Precision.HIGHEST, preferred_element_type=F32)
            total = part if total is None else total + part
        for b in range(4):
            acc[f, b] = total[:, 128 * b : 128 * b + 128]

    todo = [[0, 1], [2, 3], [4]]
    for pos in range(len(radices)):
        for f in todo[pos] if pos < 3 else []:
            volume(f)
        pair, carry = take_hops(pos, pair, carry)
        if pos + 1 < len(radices):
            start_hops(pos + 1, pair)
    for later in todo[len(radices) :]:
        for f in later:
            volume(f)

    pair = [jnp.where(is_stator, turned(p, code, False), p) for p in pair]
    arrived = jnp.concatenate(pair, axis=1)
    put = jnp.where(lane == jnp.where(sub < 4, sub * 128 + HALF, (sub - 4) * 128 + HALF - 1), 1.0, 0.0)
    first = jnp.where(sub < 4, put, 0.0), jnp.where(sub >= 4, put, 0.0)
    tn = (((0,), (0,)), ((), ()))
    spread = [
        lax.dot_general(arrived, p, tn, precision=lax.Precision.HIGHEST, preferred_element_type=F32)
        for p in first
    ]

    for end in range(2):
        span(end).wait()
    w = 0.5 * metric_scale[1] / end_weight
    for b in range(5):
        left, right = [], []
        for f in range(7):
            rows = slice(32 * f, 32 * f + 32)
            if b > 0:
                left.append(grid[1, rows, 128 * b - 128 : 128 * b])
            if b < 4:
                right.append(grid[0, rows, 128 * b : 128 * b + 128])
        for f in range(7):
            rows = slice(32 * f, 32 * f + 32)
            if b == 0:
                wall = -right[f] if f == 2 else right[f]
                left.append(jnp.where(slab > 0, sp_recv[0, rows, :], wall))
            if b == 4:
                wall = -left[f] if f == 2 else left[f]
                right.append(jnp.where(slab < nspan - 1, sp_recv[1, rows, :], wall))
        diff, jump = face_parts(left, right, 1)
        for f in range(5):
            if b > 0:
                corr[1, 32 * f : 32 * f + 32, 128 * b - 128 : 128 * b] = w * (diff[f] + jump[f])
            if b < 4:
                corr[0, 32 * f : 32 * f + 32, 128 * b : 128 * b + 128] = w * (diff[f] - jump[f])

    w = 0.5 * metric_scale[2] / end_weight
    axial = lax.broadcasted_iota(I32, (32, 128), 1)
    for s in range(4):
        cols = slice(128 * s, 128 * s + 128)
        low = [grid[2, 32 * f : 32 * f + 32, cols] for f in range(7)]
        high = [grid[3, 32 * f : 32 * f + 32, cols] for f in range(7)]
        for end in range(2):
            own, far = (high, low) if end else (low, high)
            outer = []
            for f in range(7):
                v = pltpu.roll(far[f], 127 if end else 1, axis=1)
                v = jnp.where(
                    axial == (HALF - 1 if end else HALF), spread[end][32 * f : 32 * f + 32, cols], v
                )
                edge = own[f] if f >= 5 else 0.0
                outer.append(jnp.where(axial == (127 if end else 0), edge, v))
            diff, jump = face_parts(own if end else outer, outer if end else own, 2)
            for f in range(5):
                value = diff[f] + jump[f] if end else diff[f] - jump[f]
                corr[2 + end, 32 * f : 32 * f + 32, cols] = w * value

    for kind in range(4):
        back = moved(corr[kind], table[...], transposed=True)
        grid[kind, 0:160, :] = back
    for f in range(5):
        for end in range(2):
            for i in range(5):
                rows = slice(25 * i + 20 * end, 25 * i + 20 * end + 5)
                for b in range(4):
                    cols = slice(128 * b, 128 * b + 128)
                    acc[f, b, rows, :] += grid[end, 32 * f + 5 * i : 32 * f + 5 * i + 5, cols]
            lines = pl.ds(4 * end, 25, stride=5)
            for b in range(4):
                cols = slice(128 * b, 128 * b + 128)
                acc[f, b, lines, :] = acc[f, b, lines, :] + grid[2 + end, 32 * f : 32 * f + 25, cols]

    w = 0.5 * metric_scale[0] / end_weight
    for end in range(2):
        for part in range(len(CHUNKS)):
            circ(1 - end, part).wait_recv()
            if part == 0:
                other = one_hot(recv[end, 0:1, :], NB)
                swap = lax.dot_general(other, table[...], dims, preferred_element_type=F32).astype(BF16)
        near[end] = moved(recv[end], swap)
        rows = slice(100 * end, 100 * end + 25)
        own = [cells(src, rows) for src in (0, 1, 2, 3, 4, 5, 8)]
        outer = [near[end, 1 + 25 * f : 26 + 25 * f, :] for f in range(7)]
        diff, jump = face_parts(own if end else outer, outer if end else own, 0)
        for f in range(5):
            value = diff[f] + jump[f] if end else diff[f] - jump[f]
            for b in range(4):
                acc[f, b, rows, :] += w * value[:, 128 * b : 128 * b + 128]
    for end in range(2):
        for part in range(len(CHUNKS)):
            circ(end, part).wait_send()
    for f in range(5):
        for b in range(4):
            rates[f, :, 128 * b : 128 * b + 128] = acc[f, b]


def on_device(mesh, radices, fields, section_store, mean_velocity, sound_speed, element_slot, face_turn, rotor_offset):
    nblk, nspan = mesh.shape["blk"], mesh.shape["span"]
    hop_count = sum(r - 1 for r in radices)
    anywhere = pl.BlockSpec(memory_space=pl.ANY)
    dma = pltpu.SemaphoreType.DMA
    rates = pl.pallas_call(
        functools.partial(kernel, radices, nblk, nspan),
        out_shape=jax.ShapeDtypeStruct((5, 125, NB), F32),
        in_specs=[anywhere] * 5 + [pl.BlockSpec(memory_space=pltpu.SMEM)] * 2,
        out_specs=pl.BlockSpec(memory_space=pltpu.VMEM),
        scratch_shapes=[
            pltpu.VMEM((9, 4, 125, 128), F32),
            pltpu.VMEM((5, 4, 125, 128), F32),
            pltpu.VMEM((1, NB), I32),
            pltpu.VMEM((3, 125, 125), F32),
            pltpu.VMEM((NB, NB), BF16),
            pltpu.VMEM((2, PACK_ROWS, NB), F32),
            pltpu.VMEM((2, PACK_ROWS, NB), F32),
            pltpu.VMEM((2, PACK_ROWS, NB), F32),
            pltpu.VMEM((4, 256, NB), F32),
            pltpu.VMEM((4, 256, NB), F32),
            pltpu.VMEM((4, 160, NB), F32),
            pltpu.VMEM((2, 224, 128), F32),
            pltpu.VMEM((2, 224, 128), F32),
            pltpu.VMEM((len(radices), 8, 256), F32),
            pltpu.VMEM((hop_count, 8, 256), F32),
            dma((10, 4)),
            dma((2, len(CHUNKS))),
            dma((2, len(CHUNKS))),
            dma((2,)),
            dma((2,)),
            dma((hop_count,)),
            dma((hop_count,)),
        ],
        compiler_params=pltpu.CompilerParams(
            collective_id=0, has_side_effects=True, vmem_limit_bytes=40 * 2**20
        ),
        name="rates",
    )(
        fields,
        mean_velocity,
        sound_speed,
        element_slot.reshape(1, NB),
        jnp.asarray(slope_matrices()),
        face_turn,
        rotor_offset,
    )
    store_next = section_decay * section_store + time_step * rates
    fields_next = fields + section_gain * store_next
    return fields_next, store_next


def solution(mesh, radices=RADICES):
    both = ("blk", "span")
    in_specs = (
        P(None, None, both),
        P(None, None, both),
        P(None, None, both),
        P(None, both),
        P(both),
        P("blk", "span"),
        P("span"),
    )
    return jax.shard_map(
        functools.partial(on_device, mesh, radices),
        mesh=mesh,
        in_specs=in_specs,
        out_specs=(P(None, None, both), P(None, None, both)),
        check_vma=False,
    )
```

```python
import functools

import jax
import jax.numpy as jnp
import numpy as np
from jax import lax
from jax.experimental import pallas as pl
from jax.experimental.pallas import tpu as pltpu
from jax.sharding import PartitionSpec as P

MESH = pl.DeviceIdType.MESH
F32, BF16, I32 = jnp.float32, jnp.bfloat16, jnp.int32

section_decay = -567301805773.0 / 1357537059087.0
section_gain = 5161836677717.0 / 13612068292357.0
time_step = 0.05
metric_scale = (1.0, 1.5, 0.75)
end_weight = 0.1

NB = 512
HALF = 64
RADICES = (4, 2, 4)
CHUNKS = ((0, 48), (48, 48), (96, 48), (144, 32))
PACK_ROWS = 176


def lobatto_slopes():
    root = np.sqrt(3.0 / 7.0)
    x = np.array([-1.0, -root, 0.0, root, 1.0])
    table = np.zeros((5, 5))
    for r in range(5):
        for c in range(5):
            others = [o for o in range(5) if o != r]
            if r == c:
                table[r, c] = sum(1.0 / (x[r] - x[o]) for o in others)
            else:
                top = np.prod([x[r] - x[o] for o in others])
                low = np.prod([x[c] - x[o] for o in range(5) if o != c])
                table[r, c] = top / (low * (x[r] - x[c]))
    return table


def slope_matrices():
    d, e = lobatto_slopes(), np.eye(5)
    full = [np.kron(np.kron(d, e), e), np.kron(np.kron(e, d), e), np.kron(np.kron(e, e), d)]
    return np.stack([-g * m for g, m in zip(metric_scale, full)]).astype(np.float32)


def halves(x):
    high = x.astype(BF16)
    return high, (x - high.astype(F32)).astype(BF16)


def moved(x, table, transposed=False):
    rows = x.shape[0]
    high, low = halves(x)
    both = jnp.concatenate([high, low], axis=0)
    dims = (((1,), (1 if transposed else 0,)), ((), ()))
    out = lax.dot_general(both, table, dims, preferred_element_type=F32)
    return out[:rows] + out[rows:]


def flux(q, m, c, d):
    out = [m * v for v in q]
    out[0] = out[0] + c * q[1 + d]
    out[1 + d] = out[1 + d] + c * q[4]
    out[4] = out[4] + c * q[1 + d]
    return out


def face_parts(left, right, d):
    ql, ml, cl = left[:5], left[5], left[6]
    qr, mr, cr = right[:5], right[5], right[6]
    reach = jnp.maximum(jnp.abs(ml) + cl, jnp.abs(mr) + cr)
    fl, fr = flux(ql, ml, cl, d), flux(qr, mr, cr, d)
    return [a - b for a, b in zip(fl, fr)], [reach * (b - a) for a, b in zip(ql, qr)]


def one_hot(row, count):
    k = lax.broadcasted_iota(I32, (count, row.shape[1]), 0).astype(F32)
    return jnp.where(k == row, 1.0, 0.0).astype(BF16)


def turned(x, code, inverse):
    lane = lax.broadcasted_iota(I32, (8, 128), 1)
    n = lane & 31
    i = (n * 13) >> 6
    k = n - i * 5
    ok = n < 25
    base = lane - n

    def apply(v, bit, target):
        index = jnp.where(ok, base + target, lane)
        return jnp.where((code & bit) != 0, jnp.take_along_axis(v, index, axis=1), v)

    swap, first, second = (4, k * 5 + i), (1, (4 - i) * 5 + k), (2, i * 5 + 4 - k)
    for bit, target in (second, first, swap) if inverse else (swap, first, second):
        x = apply(x, bit, target)
    return x


def kernel(
    radices,
    nblk,
    nspan,
    fields,
    mean,
    sound,
    slot_hbm,
    slopes_hbm,
    turn_hbm,
    offset_hbm,
    rates,
    turn,
    offset,
    x,
    acc,
    slot,
    slopes,
    table,
    pack,
    recv,
    near,
    face,
    grid,
    corr,
    sp_send,
    sp_recv,
    stage,
    hops,
    load_sem,
    circ_send,
    circ_recv,
    span_send,
    span_recv,
    hop_send,
    hop_recv,
):
    t = lax.axis_index("blk")
    slab = lax.axis_index("span")
    after, before = lax.rem(t + 1, nblk), lax.rem(t + nblk - 1, nblk)
    above, below = lax.rem(slab + 1, nspan), lax.rem(slab + nspan - 1, nspan)

    digits, weights, rest, weight = [], [], t, 1
    for radix in radices:
        digits.append(lax.rem(rest, radix))
        weights.append(weight)
        rest = rest // radix
        weight *= radix
    peers = []
    for pos, radix in enumerate(radices):
        for step in range(1, radix):
            to = t + (lax.rem(digits[pos] + step, radix) - digits[pos]) * weights[pos]
            peers.append((pos, step, to))

    barrier = pltpu.get_barrier_semaphore()
    for to in (after, before):
        pl.semaphore_signal(barrier, inc=1, device_id={"blk": to}, device_id_type=MESH)
    for to in (above, below):
        pl.semaphore_signal(barrier, inc=1, device_id={"span": to}, device_id_type=MESH)
    for _, _, to in peers:
        pl.semaphore_signal(barrier, inc=1, device_id={"blk": to}, device_id_type=MESH)

    def load(src):
        if src < 5:
            array = fields.at[src]
        else:
            array = mean.at[src - 5] if src < 8 else sound
        return [
            pltpu.make_async_copy(array.at[:, pl.ds(128 * b, 128)], x.at[src, b], load_sem.at[src, b])
            for b in range(4)
        ]

    def cells(src, rows=slice(0, 125)):
        return jnp.concatenate([x[src, b, rows, :] for b in range(4)], axis=1)

    load_slot = pltpu.make_async_copy(slot_hbm, slot, load_sem.at[9, 0])
    load_slopes = pltpu.make_async_copy(slopes_hbm, slopes, load_sem.at[9, 1])
    load_turn = pltpu.make_async_copy(turn_hbm, turn, load_sem.at[9, 2])
    load_offset = pltpu.make_async_copy(offset_hbm, offset, load_sem.at[9, 3])
    load_slot.start()
    for src in (0, 1, 2, 3, 4, 5, 8, 6, 7):
        for copy in load(src):
            copy.start()
    load_slopes.start()
    load_turn.start()
    load_offset.start()

    load_slot.wait()
    slot_row = slot[...].astype(F32)
    table[...] = one_hot(slot_row, NB)
    for end in range(2):
        pack[end, 0:1, :] = slot_row

    for at, src in enumerate((0, 1, 2, 3, 4, 5, 8)):
        for copy in load(src):
            copy.wait()
        for end in range(2):
            pack[end, 1 + 25 * at : 26 + 25 * at, :] = cells(src, slice(100 * end, 100 * end + 25))

    pl.semaphore_wait(barrier, 4 + len(peers))

    def circ(end, part):
        start, rows = CHUNKS[part]
        return pltpu.make_async_remote_copy(
            src_ref=pack.at[end, pl.ds(start, rows), :],
            dst_ref=recv.at[1 - end, pl.ds(start, rows), :],
            send_sem=circ_send.at[end, part],
            recv_sem=circ_recv.at[1 - end, part],
            device_id={"blk": after if end == 1 else before},
            device_id_type=MESH,
        )

    for end in range(2):
        circ(end, 0).start()

    for src in (6, 7):
        for copy in load(src):
            copy.wait()
    for d in (2, 1):
        for at, src in enumerate((0, 1, 2, 3, 4, 4 + 1 + d, 8)):
            for end in range(2):
                kind = 2 * (d - 1) + end
                if d == 2:
                    face[kind, 32 * at : 32 * at + 25, :] = cells(src, pl.ds(4 * end, 25, stride=5))
                else:
                    for i in range(5):
                        rows = slice(25 * i + 20 * end, 25 * i + 20 * end + 5)
                        face[kind, 32 * at + 5 * i : 32 * at + 5 * i + 5, :] = cells(src, rows)

    lane = lax.broadcasted_iota(I32, (8, NB), 1)
    sub = lax.broadcasted_iota(I32, (8, NB), 0)
    wanted = jnp.where(sub < 4, sub * 128 + (HALF - 1), (sub - 4) * 128 + HALF)
    column = jnp.sum(jnp.where(lane == wanted, slot_row, 0.0), axis=1, keepdims=True)
    hot = jnp.where(lane.astype(F32) == column, 1.0, 0.0)
    dims = (((1,), (1,)), ((), ()))
    packet = jnp.zeros((8, 256), F32)
    for kind, rows in ((3, sub < 4), (2, sub >= 4)):
        pick = jnp.where(rows, hot, 0.0).astype(BF16)
        for part in halves(face[kind]):
            packet = packet + lax.dot_general(pick, part, dims, preferred_element_type=F32)

    sub1 = lax.broadcasted_iota(I32, (8, 128), 0)
    row = sub1 & 3
    is_stator = sub1 < 4

    def per_row(values):
        out = jnp.full((8, 128), values[3], I32)
        for s in range(3):
            out = jnp.where(row == s, values[s], out)
        return out

    load_turn.wait()
    load_offset.wait()
    code = per_row([turn[0, s] for s in range(4)])
    shift = per_row([offset[s] for s in range(4)])
    shift = jnp.where(is_stator, shift, (nblk - shift) & (nblk - 1))
    pair = [packet[:, :128], packet[:, 128:]]
    pair = [jnp.where(is_stator, p, turned(p, code, True)) for p in pair]

    def hop(number):
        pos, step, to = peers[number]
        return pltpu.make_async_remote_copy(
            src_ref=stage.at[pos],
            dst_ref=hops.at[number],
            send_sem=hop_send.at[number],
            recv_sem=hop_recv.at[number],
            device_id={"blk": to},
            device_id_type=MESH,
        )

    def start_hops(pos, pair):
        for h in range(2):
            stage[pos, :, 128 * h : 128 * h + 128] = pair[h]
        for number, (p, _, _) in enumerate(peers):
            if p == pos:
                hop(number).start()

    start_hops(0, pair)
    for part in range(1, len(CHUNKS)):
        for end in range(2):
            circ(end, part).start()

    for kind in (1, 0):
        grid[kind] = moved(face[kind], table[...])
        sp_send[kind] = grid[kind, 0:224, 384 * kind : 384 * kind + 128]

    def span(end):
        return pltpu.make_async_remote_copy(
            src_ref=sp_send.at[end],
            dst_ref=sp_recv.at[1 - end],
            send_sem=span_send.at[end],
            recv_sem=span_recv.at[1 - end],
            device_id={"span": above if end == 1 else below},
            device_id_type=MESH,
        )

    for end in range(2):
        span(end).start()
    for kind in (2, 3):
        grid[kind] = moved(face[kind], table[...])

    carry = jnp.zeros((8, 128), I32)

    def take_hops(pos, pair, carry):
        radix = radices[pos]
        digit = lax.rem(shift // weights[pos], radix) + carry
        source = lax.rem(digits[pos] + 2 * radix - digit, radix)
        next_carry = (source + digit - digits[pos]) // radix
        distance = lax.rem(digit, radix)
        for number, (p, step, _) in enumerate(peers):
            if p == pos:
                hop(number).wait()
                for h in range(2):
                    arrived = hops[number, :, 128 * h : 128 * h + 128]
                    pair[h] = jnp.where(distance == step, arrived, pair[h])
        return pair, next_carry

    load_slopes.wait()
    velocity = (5, 6, 7)

    def volume(f):
        total = None
        for d in range(3):
            fx = cells(velocity[d]) * cells(f)
            if f == 0 or f == 4:
                fx = fx + cells(8) * cells(1 + d)
            elif f == 1 + d:
                fx = fx + cells(8) * cells(4)
            part = jnp.dot(slopes[d], fx, precision=lax.Precision.HIGHEST, preferred_element_type=F32)
            total = part if total is None else total + part
        for b in range(4):
            acc[f, b] = total[:, 128 * b : 128 * b + 128]

    todo = [[0, 1], [2, 3], [4]]
    for pos in range(len(radices)):
        for f in todo[pos] if pos < 3 else []:
            volume(f)
        pair, carry = take_hops(pos, pair, carry)
        if pos + 1 < len(radices):
            start_hops(pos + 1, pair)
    for later in todo[len(radices) :]:
        for f in later:
            volume(f)

    pair = [jnp.where(is_stator, turned(p, code, False), p) for p in pair]
    arrived = jnp.concatenate(pair, axis=1)
    put = jnp.where(lane == jnp.where(sub < 4, sub * 128 + HALF, (sub - 4) * 128 + HALF - 1), 1.0, 0.0)
    first = jnp.where(sub < 4, put, 0.0), jnp.where(sub >= 4, put, 0.0)
    tn = (((0,), (0,)), ((), ()))
    spread = [
        lax.dot_general(arrived, p, tn, precision=lax.Precision.HIGHEST, preferred_element_type=F32)
        for p in first
    ]

    for end in range(2):
        span(end).wait()
    w = 0.5 * metric_scale[1] / end_weight
    for b in range(5):
        left, right = [], []
        for f in range(7):
            rows = slice(32 * f, 32 * f + 32)
            if b > 0:
                left.append(grid[1, rows, 128 * b - 128 : 128 * b])
            if b < 4:
                right.append(grid[0, rows, 128 * b : 128 * b + 128])
        for f in range(7):
            rows = slice(32 * f, 32 * f + 32)
            if b == 0:
                wall = -right[f] if f == 2 else right[f]
                left.append(jnp.where(slab > 0, sp_recv[0, rows, :], wall))
            if b == 4:
                wall = -left[f] if f == 2 else left[f]
                right.append(jnp.where(slab < nspan - 1, sp_recv[1, rows, :], wall))
        diff, jump = face_parts(left, right, 1)
        for f in range(5):
            if b > 0:
                corr[1, 32 * f : 32 * f + 32, 128 * b - 128 : 128 * b] = w * (diff[f] + jump[f])
            if b < 4:
                corr[0, 32 * f : 32 * f + 32, 128 * b : 128 * b + 128] = w * (diff[f] - jump[f])

    w = 0.5 * metric_scale[2] / end_weight
    axial = lax.broadcasted_iota(I32, (32, 128), 1)
    for s in range(4):
        cols = slice(128 * s, 128 * s + 128)
        low = [grid[2, 32 * f : 32 * f + 32, cols] for f in range(7)]
        high = [grid[3, 32 * f : 32 * f + 32, cols] for f in range(7)]
        for end in range(2):
            own, far = (high, low) if end else (low, high)
            outer = []
            for f in range(7):
                v = pltpu.roll(far[f], 127 if end else 1, axis=1)
                v = jnp.where(
                    axial == (HALF - 1 if end else HALF), spread[end][32 * f : 32 * f + 32, cols], v
                )
                edge = own[f] if f >= 5 else 0.0
                outer.append(jnp.where(axial == (127 if end else 0), edge, v))
            diff, jump = face_parts(own if end else outer, outer if end else own, 2)
            for f in range(5):
                value = diff[f] + jump[f] if end else diff[f] - jump[f]
                corr[2 + end, 32 * f : 32 * f + 32, cols] = w * value

    for kind in range(4):
        back = moved(corr[kind], table[...], transposed=True)
        grid[kind, 0:160, :] = back
    for f in range(5):
        for end in range(2):
            for i in range(5):
                rows = slice(25 * i + 20 * end, 25 * i + 20 * end + 5)
                for b in range(4):
                    cols = slice(128 * b, 128 * b + 128)
                    acc[f, b, rows, :] += grid[end, 32 * f + 5 * i : 32 * f + 5 * i + 5, cols]
            lines = pl.ds(4 * end, 25, stride=5)
            for b in range(4):
                cols = slice(128 * b, 128 * b + 128)
                acc[f, b, lines, :] = acc[f, b, lines, :] + grid[2 + end, 32 * f : 32 * f + 25, cols]

    w = 0.5 * metric_scale[0] / end_weight
    for end in range(2):
        for part in range(len(CHUNKS)):
            circ(1 - end, part).wait_recv()
            if part == 0:
                other = one_hot(recv[end, 0:1, :], NB)
                swap = lax.dot_general(other, table[...], dims, preferred_element_type=F32).astype(BF16)
        near[end] = moved(recv[end], swap)
        rows = slice(100 * end, 100 * end + 25)
        own = [cells(src, rows) for src in (0, 1, 2, 3, 4, 5, 8)]
        outer = [near[end, 1 + 25 * f : 26 + 25 * f, :] for f in range(7)]
        diff, jump = face_parts(own if end else outer, outer if end else own, 0)
        for f in range(5):
            value = diff[f] + jump[f] if end else diff[f] - jump[f]
            for b in range(4):
                acc[f, b, rows, :] += w * value[:, 128 * b : 128 * b + 128]
    for end in range(2):
        for part in range(len(CHUNKS)):
            circ(end, part).wait_send()
    for f in range(5):
        for b in range(4):
            rates[f, :, 128 * b : 128 * b + 128] = acc[f, b]


def on_device(mesh, radices, fields, section_store, mean_velocity, sound_speed, element_slot, face_turn, rotor_offset):
    nblk, nspan = mesh.shape["blk"], mesh.shape["span"]
    hop_count = sum(r - 1 for r in radices)
    anywhere = pl.BlockSpec(memory_space=pltpu.HBM)
    dma = pltpu.SemaphoreType.DMA
    rates = pl.pallas_call(
        functools.partial(kernel, radices, nblk, nspan),
        out_shape=jax.ShapeDtypeStruct((5, 125, NB), F32),
        in_specs=[anywhere] * 7,
        out_specs=pl.BlockSpec(memory_space=pltpu.VMEM),
        scratch_shapes=[
            pltpu.SMEM((1, 4), I32),
            pltpu.SMEM((4,), I32),
            pltpu.VMEM((9, 4, 125, 128), F32),
            pltpu.VMEM((5, 4, 125, 128), F32),
            pltpu.VMEM((1, NB), I32),
            pltpu.VMEM((3, 125, 125), F32),
            pltpu.VMEM((NB, NB), BF16),
            pltpu.VMEM((2, PACK_ROWS, NB), F32),
            pltpu.VMEM((2, PACK_ROWS, NB), F32),
            pltpu.VMEM((2, PACK_ROWS, NB), F32),
            pltpu.VMEM((4, 256, NB), F32),
            pltpu.VMEM((4, 256, NB), F32),
            pltpu.VMEM((4, 160, NB), F32),
            pltpu.VMEM((2, 224, 128), F32),
            pltpu.VMEM((2, 224, 128), F32),
            pltpu.VMEM((len(radices), 8, 256), F32),
            pltpu.VMEM((hop_count, 8, 256), F32),
            dma((10, 4)),
            dma((2, len(CHUNKS))),
            dma((2, len(CHUNKS))),
            dma((2,)),
            dma((2,)),
            dma((hop_count,)),
            dma((hop_count,)),
        ],
        compiler_params=pltpu.CompilerParams(
            collective_id=0, has_side_effects=True, vmem_limit_bytes=40 * 2**20
        ),
        name="rates",
    )(
        *[
            pltpu.with_memory_space_constraint(value, pltpu.HBM)
            for value in (
                fields,
                mean_velocity,
                sound_speed,
                element_slot.reshape(1, NB),
                jnp.asarray(slope_matrices()),
                face_turn,
                rotor_offset,
            )
        ]
    )
    store_next = section_decay * section_store + time_step * rates
    fields_next = fields + section_gain * store_next
    return fields_next, store_next


def solution(mesh, radices=RADICES):
    both = ("blk", "span")
    in_specs = (
        P(None, None, both),
        P(None, None, both),
        P(None, None, both),
        P(None, both),
        P(both),
        P("blk", "span"),
        P("span"),
    )
    return jax.shard_map(
        functools.partial(on_device, mesh, radices),
        mesh=mesh,
        in_specs=in_specs,
        out_specs=(P(None, None, both), P(None, None, both)),
        check_vma=False,
    )
```

```python
import functools

import jax
import jax.numpy as jnp
import numpy as np
from jax import lax
from jax.experimental import pallas as pl
from jax.experimental.pallas import tpu as pltpu
from jax.sharding import PartitionSpec as P

MESH = pl.DeviceIdType.MESH
F32, BF16, I32 = jnp.float32, jnp.bfloat16, jnp.int32

section_decay = -567301805773.0 / 1357537059087.0
section_gain = 5161836677717.0 / 13612068292357.0
time_step = 0.05
metric_scale = (1.0, 1.5, 0.75)
end_weight = 0.1

NB = 512
HALF = 64
RADICES = (4, 2, 4)
CHUNKS = ((0, 32), (32, 64), (96, 56), (152, 24))
PACK_ROWS = 176
PACK_ORDER = (5, 8, 1, 4, 0, 2, 3)


def lobatto_slopes():
    root = np.sqrt(3.0 / 7.0)
    x = np.array([-1.0, -root, 0.0, root, 1.0])
    table = np.zeros((5, 5))
    for r in range(5):
        for c in range(5):
            others = [o for o in range(5) if o != r]
            if r == c:
                table[r, c] = sum(1.0 / (x[r] - x[o]) for o in others)
            else:
                top = np.prod([x[r] - x[o] for o in others])
                low = np.prod([x[c] - x[o] for o in range(5) if o != c])
                table[r, c] = top / (low * (x[r] - x[c]))
    return table


def slope_matrices():
    d, e = lobatto_slopes(), np.eye(5)
    full = [np.kron(np.kron(d, e), e), np.kron(np.kron(e, d), e), np.kron(np.kron(e, e), d)]
    full = np.stack([-g * m for g, m in zip(metric_scale, full)])
    high = full.astype(BF16)
    return np.stack([high, (full - high.astype(np.float64)).astype(BF16)])


def halves(x):
    high = x.astype(BF16)
    return high, (x - high.astype(F32)).astype(BF16)


def moved(x, table, transposed=False):
    rows = x.shape[0]
    high, low = halves(x)
    both = jnp.concatenate([high, low], axis=0)
    dims = (((1,), (1 if transposed else 0,)), ((), ()))
    out = lax.dot_general(both, table, dims, preferred_element_type=F32)
    return out[:rows] + out[rows:]


def reach_of(left, right):
    return jnp.maximum(jnp.abs(left[5]) + left[6], jnp.abs(right[5]) + right[6])


def face_value(left, right, d, reach, f):
    sides = []
    for q in (left, right):
        flux = q[5] * q[f]
        if f == 0 or f == 4:
            flux = flux + q[6] * q[1 + d]
        elif f == 1 + d:
            flux = flux + q[6] * q[4]
        sides.append(flux)
    return sides[0] - sides[1], reach * (right[f] - left[f])


def face_parts(left, right, d):
    reach = reach_of(left, right)
    return zip(*[face_value(left, right, d, reach, f) for f in range(5)])


def one_hot(row, count):
    k = lax.broadcasted_iota(I32, (count, row.shape[1]), 0).astype(F32)
    return jnp.where(k == row, 1.0, 0.0).astype(BF16)


def turned(x, code, inverse):
    lane = lax.broadcasted_iota(I32, (8, 128), 1)
    n = lane & 31
    i = (n * 13) >> 6
    k = n - i * 5
    ok = n < 25
    base = lane - n

    def apply(v, bit, target):
        index = jnp.where(ok, base + target, lane)
        return jnp.where((code & bit) != 0, jnp.take_along_axis(v, index, axis=1), v)

    swap, first, second = (4, k * 5 + i), (1, (4 - i) * 5 + k), (2, i * 5 + 4 - k)
    for bit, target in (second, first, swap) if inverse else (swap, first, second):
        x = apply(x, bit, target)
    return x


def kernel(
    radices,
    nblk,
    nspan,
    fields,
    mean,
    sound,
    slot_hbm,
    slopes_hbm,
    turn_hbm,
    offset_hbm,
    rates,
    turn,
    offset,
    x,
    acc,
    slot,
    slopes,
    table,
    pack,
    recv,
    near,
    face,
    grid,
    corr,
    sp_send,
    sp_recv,
    stage,
    hops,
    load_sem,
    circ_send,
    circ_recv,
    span_send,
    span_recv,
    hop_send,
    hop_recv,
    far_sem,
):
    t = lax.axis_index("blk")
    slab = lax.axis_index("span")
    after, before = lax.rem(t + 1, nblk), lax.rem(t + nblk - 1, nblk)
    above, below = lax.rem(slab + 1, nspan), lax.rem(slab + nspan - 1, nspan)

    digits, weights, rest, weight = [], [], t, 1
    for radix in radices:
        digits.append(lax.rem(rest, radix))
        weights.append(weight)
        rest = rest // radix
        weight *= radix
    peers = []
    for pos, radix in enumerate(radices):
        for step in range(1, radix):
            to = t + (lax.rem(digits[pos] + step, radix) - digits[pos]) * weights[pos]
            peers.append((pos, step, to))

    barrier = pltpu.get_barrier_semaphore()
    for to in (above, below):
        pl.semaphore_signal(barrier, inc=1, device_id={"span": to}, device_id_type=MESH)
    for _, _, to in peers:
        pl.semaphore_signal(barrier, inc=1, device_id={"blk": to}, device_id_type=MESH)

    is_first, is_last = digits[0] == 0, digits[0] == radices[0] - 1

    @pl.when(is_first)
    def _():
        pl.semaphore_signal(barrier, inc=1, device_id={"blk": before}, device_id_type=MESH)

    def load(src):
        if src < 5:
            array = fields.at[src]
        else:
            array = mean.at[src - 5] if src < 8 else sound
        return [
            pltpu.make_async_copy(array.at[:, pl.ds(128 * b, 128)], x.at[src, b], load_sem.at[src, b])
            for b in range(4)
        ]

    def cells(src, rows=slice(0, 125)):
        return jnp.concatenate([x[src, b, rows, :] for b in range(4)], axis=1)

    load_slot = pltpu.make_async_copy(slot_hbm, slot, load_sem.at[9, 0])
    load_slopes = pltpu.make_async_copy(slopes_hbm, slopes, load_sem.at[9, 1])
    load_turn = pltpu.make_async_copy(turn_hbm, turn, load_sem.at[9, 2])
    load_offset = pltpu.make_async_copy(offset_hbm, offset, load_sem.at[9, 3])
    load_slot.start()
    for src in PACK_ORDER + (7, 6):
        for copy in load(src):
            copy.start()
    load_slopes.start()
    load_turn.start()
    load_offset.start()

    load_slot.wait()
    slot_row = slot[...].astype(F32)
    table[...] = one_hot(slot_row, NB)
    for end in range(2):
        pack[end, 0:1, :] = slot_row

    for at, src in enumerate(PACK_ORDER):
        for copy in load(src):
            copy.wait()
        for end in range(2):
            pack[end, 1 + 25 * at : 26 + 25 * at, :] = cells(src, slice(100 * end, 100 * end + 25))

    pl.semaphore_wait(barrier, 2 + len(peers) + is_last.astype(I32))

    @pl.when(is_last)
    def _():
        pl.semaphore_signal(far_sem, inc=1, device_id={"blk": after}, device_id_type=MESH)


    def circ(end, part):
        start, rows = CHUNKS[part]
        return pltpu.make_async_remote_copy(
            src_ref=pack.at[end, pl.ds(start, rows), :],
            dst_ref=recv.at[1 - end, pl.ds(start, rows), :],
            send_sem=circ_send.at[end, part],
            recv_sem=circ_recv.at[1 - end, part],
            device_id={"blk": after if end == 1 else before},
            device_id_type=MESH,
        )

    def start_circ(*parts):
        for part in parts:
            circ(1, part).start()

            @pl.when(jnp.logical_not(is_first))
            def _():
                circ(0, part).start()

    def start_far(*parts):
        @pl.when(is_first)
        def _():
            if parts[0] == 0:
                pl.semaphore_wait(far_sem, 1)
            for part in parts:
                circ(0, part).start()

    start_circ(0)

    for src in (6, 7):
        for copy in load(src):
            copy.wait()
    for d in (2, 1):
        for at, src in enumerate((0, 1, 2, 3, 4, 4 + 1 + d, 8)):
            for end in range(2):
                kind = 2 * (d - 1) + end
                if d == 2:
                    face[kind, 32 * at : 32 * at + 25, :] = cells(src, pl.ds(4 * end, 25, stride=5))
                else:
                    for i in range(5):
                        rows = slice(25 * i + 20 * end, 25 * i + 20 * end + 5)
                        face[kind, 32 * at + 5 * i : 32 * at + 5 * i + 5, :] = cells(src, rows)

    lane = lax.broadcasted_iota(I32, (8, NB), 1)
    sub = lax.broadcasted_iota(I32, (8, NB), 0)
    wanted = jnp.where(sub < 4, sub * 128 + (HALF - 1), (sub - 4) * 128 + HALF)
    column = jnp.sum(jnp.where(lane == wanted, slot_row, 0.0), axis=1, keepdims=True)
    hot = jnp.where(lane.astype(F32) == column, 1.0, 0.0)
    dims = (((1,), (1,)), ((), ()))
    packet = jnp.zeros((8, 256), F32)
    for kind, rows in ((3, sub < 4), (2, sub >= 4)):
        pick = jnp.where(rows, hot, 0.0).astype(BF16)
        for part in halves(face[kind]):
            packet = packet + lax.dot_general(pick, part, dims, preferred_element_type=F32)

    sub1 = lax.broadcasted_iota(I32, (8, 128), 0)
    row = sub1 & 3
    is_stator = sub1 < 4

    def per_row(values):
        out = jnp.full((8, 128), values[3], I32)
        for s in range(3):
            out = jnp.where(row == s, values[s], out)
        return out

    load_turn.wait()
    load_offset.wait()
    code = per_row([turn[0, s] for s in range(4)])
    shift = per_row([offset[s] for s in range(4)])
    shift = jnp.where(is_stator, shift, (nblk - shift) & (nblk - 1))
    own_pair = [packet[:, :128], packet[:, 128:]]
    pair = [jnp.where(is_stator, p, turned(p, code, True)) for p in own_pair]

    def hop(number):
        pos, step, to = peers[number]
        return pltpu.make_async_remote_copy(
            src_ref=stage.at[pos],
            dst_ref=hops.at[number],
            send_sem=hop_send.at[number],
            recv_sem=hop_recv.at[number],
            device_id={"blk": to},
            device_id_type=MESH,
        )

    def start_hops(pos, pair):
        for h in range(2):
            stage[pos, :, 128 * h : 128 * h + 128] = pair[h]
        for number, (p, _, _) in enumerate(peers):
            if p == pos:
                hop(number).start()

    def take_hops(pos, pair, distance):
        for number, (p, step, _) in enumerate(peers):
            if p == pos:
                hop(number).wait()
                for h in range(2):
                    arrived = hops[number, :, 128 * h : 128 * h + 128]
                    pair[h] = jnp.where(distance == step, arrived, pair[h])
        return pair

    r0, r1, r2 = radices
    shift0 = lax.rem(shift, r0)
    shift1 = lax.rem(shift // r0, r1)
    move1 = lax.rem(shift1 + (digits[0] + shift0) // r0, r1)
    carry0 = jnp.where(digits[0] < shift0, 1, 0)
    source1 = lax.rem(digits[1] + 2 * r1 - shift1 - carry0, r1)
    move2 = lax.rem(shift // (r0 * r1) + (source1 + shift1 + carry0) // r1, r2)

    start_hops(1, pair)

    @pl.when(jnp.logical_not(is_last))
    def _():
        circ(1, 1).start()

    @pl.when(jnp.logical_not(is_first))
    def _():
        circ(0, 1).start()


    for kind in (1, 0):
        grid[kind] = moved(face[kind], table[...])
        sp_send[kind] = grid[kind, 0:224, 384 * kind : 384 * kind + 128]


    def span(end):
        return pltpu.make_async_remote_copy(
            src_ref=sp_send.at[end],
            dst_ref=sp_recv.at[1 - end],
            send_sem=span_send.at[end],
            recv_sem=span_recv.at[1 - end],
            device_id={"span": above if end == 1 else below},
            device_id_type=MESH,
        )

    for end in range(2):
        span(end).start()
    for kind in (2, 3):
        grid[kind] = moved(face[kind], table[...])

    load_slopes.wait()
    velocity = (5, 6, 7)

    def volume(f):
        total = None
        for d in range(3):
            fx = cells(velocity[d]) * cells(f)
            if f == 0 or f == 4:
                fx = fx + cells(8) * cells(1 + d)
            elif f == 1 + d:
                fx = fx + cells(8) * cells(4)
            high, low = halves(fx)
            for m, v in ((0, high), (0, low), (1, high)):
                part = jnp.dot(slopes[m, d], v, preferred_element_type=F32)
                total = part if total is None else total + part
        for b in range(4):
            acc[f, b] = total[:, 128 * b : 128 * b + 128]

    volume(0)
    volume(1)
    pair = take_hops(1, pair, move1)
    start_hops(0, pair)

    @pl.when(is_last)
    def _():
        circ(1, 1).start()

    start_circ(2, 3)
    start_far(0, 1)
    for f in (2, 3, 4):
        volume(f)
    pair = take_hops(0, pair, shift0)
    start_hops(2, pair)
    start_far(2, 3)

    for end in range(2):
        span(end).wait()
    w = 0.5 * metric_scale[1] / end_weight
    for b in range(5):
        left, right = [], []
        for f in range(7):
            rows = slice(32 * f, 32 * f + 32)
            if b > 0:
                left.append(grid[1, rows, 128 * b - 128 : 128 * b])
            if b < 4:
                right.append(grid[0, rows, 128 * b : 128 * b + 128])
        for f in range(7):
            rows = slice(32 * f, 32 * f + 32)
            if b == 0:
                wall = -right[f] if f == 2 else right[f]
                left.append(jnp.where(slab > 0, sp_recv[0, rows, :], wall))
            if b == 4:
                wall = -left[f] if f == 2 else left[f]
                right.append(jnp.where(slab < nspan - 1, sp_recv[1, rows, :], wall))
        diff, jump = face_parts(left, right, 1)
        for f in range(5):
            if b > 0:
                corr[1, 32 * f : 32 * f + 32, 128 * b - 128 : 128 * b] = w * (diff[f] + jump[f])
            if b < 4:
                corr[0, 32 * f : 32 * f + 32, 128 * b : 128 * b + 128] = w * (diff[f] - jump[f])

    w = 0.5 * metric_scale[2] / end_weight
    axial = lax.broadcasted_iota(I32, (32, 128), 1)
    for s in range(4):
        cols = slice(128 * s, 128 * s + 128)
        low = [grid[2, 32 * f : 32 * f + 32, cols] for f in range(7)]
        high = [grid[3, 32 * f : 32 * f + 32, cols] for f in range(7)]
        for end in range(2):
            own, far = (high, low) if end else (low, high)
            outer = []
            for f in range(7):
                v = pltpu.roll(far[f], 127 if end else 1, axis=1)
                edge = own[f] if f >= 5 else 0.0
                outer.append(jnp.where(axial == (127 if end else 0), edge, v))
            diff, jump = face_parts(own if end else outer, outer if end else own, 2)
            slides = axial == (HALF - 1 if end else HALF)
            for f in range(5):
                value = diff[f] + jump[f] if end else diff[f] - jump[f]
                corr[2 + end, 32 * f : 32 * f + 32, cols] = jnp.where(slides, 0.0, w * value)

    def add_axial(end, values):
        for f in range(5):
            lines = pl.ds(4 * end, 25, stride=5)
            for b in range(4):
                part = values[32 * f : 32 * f + 25, 128 * b : 128 * b + 128]
                acc[f, b, lines, :] = acc[f, b, lines, :] + part

    for end in range(2):
        back = moved(corr[end], table[...], transposed=True)
        for f in range(5):
            for i in range(5):
                rows = slice(25 * i + 20 * end, 25 * i + 20 * end + 5)
                for b in range(4):
                    part = back[32 * f + 5 * i : 32 * f + 5 * i + 5, 128 * b : 128 * b + 128]
                    acc[f, b, rows, :] += part
    for end in range(2):
        add_axial(end, moved(corr[2 + end], table[...], transposed=True))

    swaps = []
    for end in range(2):
        circ(1 - end, 0).wait_recv()
        other = one_hot(recv[end, 0:1, :], NB)
        swap = lax.dot_general(other, table[...], dims, preferred_element_type=F32)
        swaps.append(swap.astype(BF16))
    weight0 = 0.5 * metric_scale[0] / end_weight
    sides = [None, None]

    def settle(fields):
        for end in range(2):
            left, right, reach = sides[end]
            rows = slice(100 * end, 100 * end + 25)
            for f in fields:
                diff, jump = face_value(left, right, 0, reach, f)
                value = weight0 * (diff + jump if end else diff - jump)
                for b in range(4):
                    acc[f, b, rows, :] += value[:, 128 * b : 128 * b + 128]

    def far_value(end, src):
        at = PACK_ORDER.index(src)
        return near[end, 1 + 25 * at : 26 + 25 * at, :]

    def settle_rows(parts):
        start, stop = CHUNKS[parts[0]][0], sum(CHUNKS[parts[-1]])
        for end in range(2):
            for part in parts:
                if part > 0:
                    circ(1 - end, part).wait_recv()
            near[end, start:stop, :] = moved(recv[end, start:stop, :], swaps[end])

    settle_rows((0, 1, 2))
    for end in range(2):
        rows = slice(100 * end, 100 * end + 25)
        order = (0, 1, 2, 3, 4, 5, 8)
        own = [cells(src, rows) for src in order]
        other = [None if src == 3 else far_value(end, src) for src in order]
        left, right = (own, other) if end else (other, own)
        sides[end] = left, right, reach_of(left, right)
    settle((0, 1, 2, 4))
    pair = take_hops(2, pair, move2)
    pair = [jnp.where(is_stator, turned(p, code, False), p) for p in pair]
    outer = [pltpu.roll(p, 4, axis=0) for p in pair]
    left = [jnp.where(is_stator, a, b) for a, b in zip(own_pair, outer)]
    right = [jnp.where(is_stator, b, a) for a, b in zip(own_pair, outer)]

    def values(pair):
        return [pair[f // 4][:, 32 * (f % 4) : 32 * (f % 4) + 32] for f in range(7)]

    diff, jump = face_parts(values(left), values(right), 2)
    sign = jnp.where(is_stator[:, :32], w, -w)
    fixes = jnp.concatenate([w * d + sign * j for d, j in zip(diff, jump)], axis=1)
    fixes = jnp.concatenate(halves(fixes), axis=0)
    tn = (((0,), (0,)), ((), ()))
    for end in range(2):
        mine = jnp.where(sub < 4 if end else sub >= 4, hot, 0.0).astype(BF16)
        spread = lax.dot_general(
            fixes, jnp.concatenate([mine, mine], axis=0), tn, preferred_element_type=F32
        )
        add_axial(end, spread)

    settle_rows((3,))
    for end in range(2):
        sides[end][1 if end else 0][3] = far_value(end, 3)
    settle((3,))
    for f in range(5):
        for b in range(4):
            rates[f, :, 128 * b : 128 * b + 128] = acc[f, b]
    for end in range(2):
        for part in range(len(CHUNKS)):
            circ(end, part).wait_send()


def on_device(mesh, radices, fields, section_store, mean_velocity, sound_speed, element_slot, face_turn, rotor_offset):
    nblk, nspan = mesh.shape["blk"], mesh.shape["span"]
    hop_count = sum(r - 1 for r in radices)
    anywhere = pl.BlockSpec(memory_space=pltpu.HBM)
    dma = pltpu.SemaphoreType.DMA
    rates = pl.pallas_call(
        functools.partial(kernel, radices, nblk, nspan),
        out_shape=jax.ShapeDtypeStruct((5, 125, NB), F32),
        in_specs=[anywhere] * 7,
        out_specs=pl.BlockSpec(memory_space=pltpu.VMEM),
        scratch_shapes=[
            pltpu.SMEM((1, 4), I32),
            pltpu.SMEM((4,), I32),
            pltpu.VMEM((9, 4, 125, 128), F32),
            pltpu.VMEM((5, 4, 125, 128), F32),
            pltpu.VMEM((1, NB), I32),
            pltpu.VMEM((2, 3, 125, 125), BF16),
            pltpu.VMEM((NB, NB), BF16),
            pltpu.VMEM((2, PACK_ROWS, NB), F32),
            pltpu.VMEM((2, PACK_ROWS, NB), F32),
            pltpu.VMEM((2, PACK_ROWS, NB), F32),
            pltpu.VMEM((4, 256, NB), F32),
            pltpu.VMEM((4, 256, NB), F32),
            pltpu.VMEM((4, 160, NB), F32),
            pltpu.VMEM((2, 224, 128), F32),
            pltpu.VMEM((2, 224, 128), F32),
            pltpu.VMEM((len(radices), 8, 256), F32),
            pltpu.VMEM((hop_count, 8, 256), F32),
            dma((10, 4)),
            dma((2, len(CHUNKS))),
            dma((2, len(CHUNKS))),
            dma((2,)),
            dma((2,)),
            dma((hop_count,)),
            dma((hop_count,)),
            pltpu.SemaphoreType.REGULAR,
        ],
        compiler_params=pltpu.CompilerParams(
            collective_id=0, has_side_effects=True, vmem_limit_bytes=40 * 2**20
        ),
        name="rates",
    )(
        *[
            pltpu.with_memory_space_constraint(value, pltpu.HBM)
            for value in (
                fields,
                mean_velocity,
                sound_speed,
                element_slot.reshape(1, NB),
                jnp.asarray(slope_matrices()),
                face_turn,
                rotor_offset,
            )
        ]
    )
    store_next = section_decay * section_store + time_step * rates
    fields_next = fields + section_gain * store_next
    return fields_next, store_next


def solution(mesh, radices=RADICES):
    both = ("blk", "span")
    in_specs = (
        P(None, None, both),
        P(None, None, both),
        P(None, None, both),
        P(None, both),
        P(both),
        P("blk", "span"),
        P("span"),
    )
    return jax.shard_map(
        functools.partial(on_device, mesh, radices),
        mesh=mesh,
        in_specs=in_specs,
        out_specs=(P(None, None, both), P(None, None, both)),
        check_vma=False,
    )
```

```python
import functools

import jax
import jax.numpy as jnp
import numpy as np
from jax import lax
from jax.experimental import pallas as pl
from jax.experimental.pallas import tpu as pltpu
from jax.sharding import PartitionSpec as P

MESH = pl.DeviceIdType.MESH
F32, BF16, I32 = jnp.float32, jnp.bfloat16, jnp.int32

section_decay = -567301805773.0 / 1357537059087.0
section_gain = 5161836677717.0 / 13612068292357.0
time_step = 0.05
metric_scale = (1.0, 1.5, 0.75)
end_weight = 0.1

NB = 512
HALF = 64
RADICES = (4, 2, 4)
CHUNKS = ((0, 32), (32, 64), (96, 56), (152, 24))
PACK_ROWS = 176
PACK_ORDER = (5, 8, 1, 4, 0, 2, 3)


def lobatto_slopes():
    root = np.sqrt(3.0 / 7.0)
    x = np.array([-1.0, -root, 0.0, root, 1.0])
    table = np.zeros((5, 5))
    for r in range(5):
        for c in range(5):
            others = [o for o in range(5) if o != r]
            if r == c:
                table[r, c] = sum(1.0 / (x[r] - x[o]) for o in others)
            else:
                top = np.prod([x[r] - x[o] for o in others])
                low = np.prod([x[c] - x[o] for o in range(5) if o != c])
                table[r, c] = top / (low * (x[r] - x[c]))
    return table


def slope_matrices():
    d, e = lobatto_slopes(), np.eye(5)
    full = [np.kron(np.kron(d, e), e), np.kron(np.kron(e, d), e), np.kron(np.kron(e, e), d)]
    full = np.stack([-g * m for g, m in zip(metric_scale, full)])
    high = full.astype(BF16)
    return np.stack([high, (full - high.astype(np.float64)).astype(BF16)])


def halves(x):
    high = x.astype(BF16)
    return high, (x - high.astype(F32)).astype(BF16)


def moved(x, table, transposed=False):
    rows = x.shape[0]
    high, low = halves(x)
    both = jnp.concatenate([high, low], axis=0)
    dims = (((1,), (1 if transposed else 0,)), ((), ()))
    out = lax.dot_general(both, table, dims, preferred_element_type=F32)
    return out[:rows] + out[rows:]


def reach_of(left, right):
    return jnp.maximum(jnp.abs(left[5]) + left[6], jnp.abs(right[5]) + right[6])


def face_value(left, right, d, reach, f):
    sides = []
    for q in (left, right):
        flux = q[5] * q[f]
        if f == 0 or f == 4:
            flux = flux + q[6] * q[1 + d]
        elif f == 1 + d:
            flux = flux + q[6] * q[4]
        sides.append(flux)
    return sides[0] - sides[1], reach * (right[f] - left[f])


def face_parts(left, right, d):
    reach = reach_of(left, right)
    return zip(*[face_value(left, right, d, reach, f) for f in range(5)])


def one_hot(row, count):
    k = lax.broadcasted_iota(I32, (count, row.shape[1]), 0).astype(F32)
    return jnp.where(k == row, 1.0, 0.0).astype(BF16)


def turned(x, code, inverse):
    lane = lax.broadcasted_iota(I32, (8, 128), 1)
    n = lane & 31
    i = (n * 13) >> 6
    k = n - i * 5
    ok = n < 25
    base = lane - n

    def apply(v, bit, target):
        index = jnp.where(ok, base + target, lane)
        return jnp.where((code & bit) != 0, jnp.take_along_axis(v, index, axis=1), v)

    swap, first, second = (4, k * 5 + i), (1, (4 - i) * 5 + k), (2, i * 5 + 4 - k)
    for bit, target in (second, first, swap) if inverse else (swap, first, second):
        x = apply(x, bit, target)
    return x


def kernel(
    radices,
    nblk,
    nspan,
    fields,
    mean,
    sound,
    slot_hbm,
    slopes_hbm,
    turn_hbm,
    offset_hbm,
    rates,
    turn,
    offset,
    x,
    acc,
    slot,
    slopes,
    table,
    pack,
    recv,
    near,
    face,
    grid,
    corr,
    sp_send,
    sp_recv,
    own_packet,
    gathered,
    bundle,
    hops,
    final_out,
    final_in,
    load_sem,
    circ_send,
    circ_recv,
    span_send,
    span_recv,
    hop_send,
    hop_recv,
    plane_send,
    plane_recv,
    far_sem,
):
    t = lax.axis_index("blk")
    slab = lax.axis_index("span")
    after, before = lax.rem(t + 1, nblk), lax.rem(t + nblk - 1, nblk)
    above, below = lax.rem(slab + 1, nspan), lax.rem(slab + nspan - 1, nspan)

    r0, r1, r2 = radices
    z, y, x_at = lax.rem(t, r0), lax.rem(t // r0, r1), t // (r0 * r1)
    is_first, is_last = z == 0, z == r0 - 1
    inner = jnp.logical_and(z > 0, z < r0 - 1)
    run = [t + (lax.rem(z + step, r0) - z) for step in range(1, r0)]
    across = [jnp.logical_and(z == 0, step == r0 - 1) | jnp.logical_and(z == r0 - 1, step == 1) for step in range(1, r0)]
    plane = []
    for dy in range(r1):
        for dx in range(r2):
            if dy or dx:
                to = z + r0 * lax.rem(y + dy, r1) + r0 * r1 * lax.rem(x_at + dx, r2)
                plane.append((dy, dx, to))

    barrier = pltpu.get_barrier_semaphore()
    for to in (above, below):
        pl.semaphore_signal(barrier, inc=1, device_id={"span": to}, device_id_type=MESH)
    for to, skip in zip(run, across):

        @pl.when(jnp.logical_not(skip))
        def _():
            pl.semaphore_signal(barrier, inc=1, device_id={"blk": to}, device_id_type=MESH)

    @pl.when(inner)
    def _():
        for _, _, to in plane:
            pl.semaphore_signal(barrier, inc=1, device_id={"blk": to}, device_id_type=MESH)

    @pl.when(is_first)
    def _():
        pl.semaphore_signal(barrier, inc=1, device_id={"blk": before}, device_id_type=MESH)

    def load(src):
        if src < 5:
            array = fields.at[src]
        else:
            array = mean.at[src - 5] if src < 8 else sound
        return [
            pltpu.make_async_copy(array.at[:, pl.ds(128 * b, 128)], x.at[src, b], load_sem.at[src, b])
            for b in range(4)
        ]

    def cells(src, rows=slice(0, 125)):
        return jnp.concatenate([x[src, b, rows, :] for b in range(4)], axis=1)

    load_slot = pltpu.make_async_copy(slot_hbm, slot, load_sem.at[9, 0])
    load_slopes = pltpu.make_async_copy(slopes_hbm, slopes, load_sem.at[9, 1])
    load_turn = pltpu.make_async_copy(turn_hbm, turn, load_sem.at[9, 2])
    load_offset = pltpu.make_async_copy(offset_hbm, offset, load_sem.at[9, 3])
    load_slot.start()
    for src in PACK_ORDER + (7, 6):
        for copy in load(src):
            copy.start()
    load_slopes.start()
    load_turn.start()
    load_offset.start()

    load_slot.wait()
    slot_row = slot[...].astype(F32)
    table[...] = one_hot(slot_row, NB)
    for end in range(2):
        pack[end, 0:1, :] = slot_row

    lane = lax.broadcasted_iota(I32, (8, NB), 1)
    sub = lax.broadcasted_iota(I32, (8, NB), 0)
    wanted = jnp.where(sub < 4, sub * 128 + (HALF - 1), (sub - 4) * 128 + HALF)
    column = jnp.sum(jnp.where(lane == wanted, slot_row, 0.0), axis=1, keepdims=True)
    hot = jnp.where(lane.astype(F32) == column, 1.0, 0.0)

    for at, src in enumerate(PACK_ORDER):
        for copy in load(src):
            copy.wait()
        for end in range(2):
            pack[end, 1 + 25 * at : 26 + 25 * at, :] = cells(src, slice(100 * end, 100 * end + 25))

    pl.semaphore_wait(barrier, jnp.where(inner, 2 + r0 - 1 + len(plane), r0 + is_last.astype(I32)))

    @pl.when(is_last)
    def _():
        pl.semaphore_signal(far_sem, inc=1, device_id={"blk": after}, device_id_type=MESH)


    def circ(end, part):
        start, rows = CHUNKS[part]
        return pltpu.make_async_remote_copy(
            src_ref=pack.at[end, pl.ds(start, rows), :],
            dst_ref=recv.at[1 - end, pl.ds(start, rows), :],
            send_sem=circ_send.at[end, part],
            recv_sem=circ_recv.at[1 - end, part],
            device_id={"blk": after if end == 1 else before},
            device_id_type=MESH,
        )

    def start_circ(*parts):
        for part in parts:

            @pl.when(jnp.logical_not(is_last))
            def _():
                circ(1, part).start()

            @pl.when(jnp.logical_not(is_first))
            def _():
                circ(0, part).start()

    every = range(len(CHUNKS))

    @pl.when(is_last)
    def _():
        for part in every:
            circ(1, part).start()

    start_circ(0)

    for src in (6, 7):
        for copy in load(src):
            copy.wait()
    for d in (2, 1):
        for at, src in enumerate((0, 1, 2, 3, 4, 4 + 1 + d, 8)):
            for end in range(2):
                kind = 2 * (d - 1) + end
                if d == 2:
                    face[kind, 32 * at : 32 * at + 25, :] = cells(src, pl.ds(4 * end, 25, stride=5))
                else:
                    for i in range(5):
                        rows = slice(25 * i + 20 * end, 25 * i + 20 * end + 5)
                        face[kind, 32 * at + 5 * i : 32 * at + 5 * i + 5, :] = cells(src, rows)

    dims = (((1,), (1,)), ((), ()))
    packet = jnp.zeros((8, 256), F32)
    for kind, rows in ((3, sub < 4), (2, sub >= 4)):
        pick = jnp.where(rows, hot, 0.0).astype(BF16)
        for part in halves(face[kind]):
            packet = packet + lax.dot_general(pick, part, dims, preferred_element_type=F32)

    sub1 = lax.broadcasted_iota(I32, (8, 128), 0)
    row = sub1 & 3
    is_stator = sub1 < 4

    def per_row(values):
        out = jnp.full((8, 128), values[3], I32)
        for s in range(3):
            out = jnp.where(row == s, values[s], out)
        return out

    load_turn.wait()
    load_offset.wait()
    code = per_row([turn[0, s] for s in range(4)])
    shift = per_row([offset[s] for s in range(4)])
    shift = jnp.where(is_stator, shift, (nblk - shift) & (nblk - 1))
    own_pair = [packet[:, :128], packet[:, 128:]]
    pair = [jnp.where(is_stator, p, turned(p, code, True)) for p in own_pair]

    for h in range(2):
        own_packet[:, 128 * h : 128 * h + 128] = pair[h]

    def collect(to_z, from_z):
        return pltpu.make_async_remote_copy(
            src_ref=own_packet,
            dst_ref=gathered.at[from_z],
            send_sem=hop_send.at[to_z],
            recv_sem=hop_recv.at[from_z],
            device_id={"blk": t + to_z - z},
            device_id_type=MESH,
        )

    for to_z in range(1, r0 - 1):

        @pl.when(z != to_z)
        def _():
            collect(to_z, z).start()

    start_circ(1, 2, 3)

    def take_collected():
        @pl.when(inner)
        def _():
            for from_z in range(r0):

                @pl.when(z != from_z)
                def _():
                    collect(1, from_z).wait_recv()

        for to_z in range(1, r0 - 1):

            @pl.when(z != to_z)
            def _():
                collect(to_z, 0).wait_send()

        for h in range(2):
            lanes = slice(128 * h, 128 * h + 128)
            for half, target in enumerate((z, outer_z)):
                source = lax.rem(target + r0 - shift0, r0)
                value = pair[h]
                for from_z in range(r0):
                    value = jnp.where((source == from_z) & (z != from_z), gathered[from_z, :, lanes], value)
                bundle[8 * half : 8 * half + 8, lanes] = value

    outer_z = jnp.where(z == 1, 0, r0 - 1)
    shift0 = lax.rem(shift, r0)
    shift1 = lax.rem(shift // r0, r1)
    shift2 = shift // (r0 * r1)

    def hop(number):
        return pltpu.make_async_remote_copy(
            src_ref=bundle,
            dst_ref=hops.at[number],
            send_sem=plane_send.at[number],
            recv_sem=plane_recv.at[number],
            device_id={"blk": plane[number][2]},
            device_id_type=MESH,
        )

    def start_plane():
        @pl.when(inner)
        def _():
            for number in range(len(plane)):
                hop(number).start()

    def take_plane():
        @pl.when(inner)
        def _():
            for number in range(len(plane)):
                hop(number).wait()

        for half, target in enumerate((z, outer_z)):
            up1 = shift1 + jnp.where(target < shift0, 1, 0)
            source1 = lax.rem(y + 2 * r1 - up1, r1)
            move1 = lax.rem(up1, r1)
            move2 = lax.rem(shift2 + (source1 + up1) // r1, r2)
            for h in range(2):
                lanes = slice(128 * h, 128 * h + 128)
                rows = slice(8 * half, 8 * half + 8)
                value = bundle[rows, lanes]
                for number, (dy, dx, _) in enumerate(plane):
                    value = jnp.where((move1 == dy) & (move2 == dx), hops[number, rows, lanes], value)
                final_out[half, :, lanes] = value

    def deliver():
        return pltpu.make_async_remote_copy(
            src_ref=final_out.at[1],
            dst_ref=final_in,
            send_sem=hop_send.at[0],
            recv_sem=hop_send.at[r0 - 1],
            device_id={"blk": lax.rem(t + jnp.where(z == 1, nblk - 1, 1), nblk)},
            device_id_type=MESH,
        )

    for kind in (1, 0):
        grid[kind] = moved(face[kind], table[...])
        sp_send[kind] = grid[kind, 0:224, 384 * kind : 384 * kind + 128]


    def span(end):
        return pltpu.make_async_remote_copy(
            src_ref=sp_send.at[end],
            dst_ref=sp_recv.at[1 - end],
            send_sem=span_send.at[end],
            recv_sem=span_recv.at[1 - end],
            device_id={"span": above if end == 1 else below},
            device_id_type=MESH,
        )

    for end in range(2):
        span(end).start()
    for kind in (2, 3):
        grid[kind] = moved(face[kind], table[...])

    load_slopes.wait()
    velocity = (5, 6, 7)

    def volume(f):
        total = None
        for d in range(3):
            fx = cells(velocity[d]) * cells(f)
            if f == 0 or f == 4:
                fx = fx + cells(8) * cells(1 + d)
            elif f == 1 + d:
                fx = fx + cells(8) * cells(4)
            high, low = halves(fx)
            for m, v in ((0, high), (0, low), (1, high)):
                part = jnp.dot(slopes[m, d], v, preferred_element_type=F32)
                total = part if total is None else total + part
        for b in range(4):
            acc[f, b] = total[:, 128 * b : 128 * b + 128]

    volume(0)
    volume(1)
    take_collected()
    start_plane()

    @pl.when(is_first)
    def _():
        pl.semaphore_wait(far_sem, 1)
        for part in every:
            circ(0, part).start()

    for f in (2, 3, 4):
        volume(f)

    for end in range(2):
        span(end).wait()
    w = 0.5 * metric_scale[1] / end_weight
    for b in range(5):
        left, right = [], []
        for f in range(7):
            rows = slice(32 * f, 32 * f + 32)
            if b > 0:
                left.append(grid[1, rows, 128 * b - 128 : 128 * b])
            if b < 4:
                right.append(grid[0, rows, 128 * b : 128 * b + 128])
        for f in range(7):
            rows = slice(32 * f, 32 * f + 32)
            if b == 0:
                wall = -right[f] if f == 2 else right[f]
                left.append(jnp.where(slab > 0, sp_recv[0, rows, :], wall))
            if b == 4:
                wall = -left[f] if f == 2 else left[f]
                right.append(jnp.where(slab < nspan - 1, sp_recv[1, rows, :], wall))
        diff, jump = face_parts(left, right, 1)
        for f in range(5):
            if b > 0:
                corr[1, 32 * f : 32 * f + 32, 128 * b - 128 : 128 * b] = w * (diff[f] + jump[f])
            if b < 4:
                corr[0, 32 * f : 32 * f + 32, 128 * b : 128 * b + 128] = w * (diff[f] - jump[f])

    w = 0.5 * metric_scale[2] / end_weight
    axial = lax.broadcasted_iota(I32, (32, 128), 1)
    for s in range(4):
        cols = slice(128 * s, 128 * s + 128)
        low = [grid[2, 32 * f : 32 * f + 32, cols] for f in range(7)]
        high = [grid[3, 32 * f : 32 * f + 32, cols] for f in range(7)]
        for end in range(2):
            own, far = (high, low) if end else (low, high)
            outer = []
            for f in range(7):
                v = pltpu.roll(far[f], 127 if end else 1, axis=1)
                edge = own[f] if f >= 5 else 0.0
                outer.append(jnp.where(axial == (127 if end else 0), edge, v))
            diff, jump = face_parts(own if end else outer, outer if end else own, 2)
            slides = axial == (HALF - 1 if end else HALF)
            for f in range(5):
                value = diff[f] + jump[f] if end else diff[f] - jump[f]
                corr[2 + end, 32 * f : 32 * f + 32, cols] = jnp.where(slides, 0.0, w * value)

    def add_axial(end, values):
        for f in range(5):
            lines = pl.ds(4 * end, 25, stride=5)
            for b in range(4):
                part = values[32 * f : 32 * f + 25, 128 * b : 128 * b + 128]
                acc[f, b, lines, :] = acc[f, b, lines, :] + part

    for end in range(2):
        back = moved(corr[end], table[...], transposed=True)
        for f in range(5):
            for i in range(5):
                rows = slice(25 * i + 20 * end, 25 * i + 20 * end + 5)
                for b in range(4):
                    part = back[32 * f + 5 * i : 32 * f + 5 * i + 5, 128 * b : 128 * b + 128]
                    acc[f, b, rows, :] += part
    for end in range(2):
        add_axial(end, moved(corr[2 + end], table[...], transposed=True))

    swaps = []
    for end in range(2):
        circ(1 - end, 0).wait_recv()
        other = one_hot(recv[end, 0:1, :], NB)
        swap = lax.dot_general(other, table[...], dims, preferred_element_type=F32)
        swaps.append(swap.astype(BF16))
    weight0 = 0.5 * metric_scale[0] / end_weight
    sides = [None, None]

    def settle(fields):
        for end in range(2):
            left, right, reach = sides[end]
            rows = slice(100 * end, 100 * end + 25)
            for f in fields:
                diff, jump = face_value(left, right, 0, reach, f)
                value = weight0 * (diff + jump if end else diff - jump)
                for b in range(4):
                    acc[f, b, rows, :] += value[:, 128 * b : 128 * b + 128]

    def far_value(end, src):
        at = PACK_ORDER.index(src)
        return near[end, 1 + 25 * at : 26 + 25 * at, :]

    def settle_rows(parts):
        start, stop = CHUNKS[parts[0]][0], sum(CHUNKS[parts[-1]])
        for end in range(2):
            for part in parts:
                if part > 0:
                    circ(1 - end, part).wait_recv()
            near[end, start:stop, :] = moved(recv[end, start:stop, :], swaps[end])

    take_plane()

    @pl.when(inner)
    def _():
        deliver().start()

    settle_rows((0, 1, 2))
    for end in range(2):
        rows = slice(100 * end, 100 * end + 25)
        order = (0, 1, 2, 3, 4, 5, 8)
        own = [cells(src, rows) for src in order]
        other = [None if src == 3 else far_value(end, src) for src in order]
        left, right = (own, other) if end else (other, own)
        sides[end] = left, right, reach_of(left, right)
    settle((0, 1, 2, 4))
    settle_rows((3,))
    for end in range(2):
        sides[end][1 if end else 0][3] = far_value(end, 3)
    settle((3,))
    @pl.when(jnp.logical_not(inner))
    def _():
        deliver().wait_recv()

    pair = []
    for h in range(2):
        lanes = slice(128 * h, 128 * h + 128)
        pair.append(jnp.where(inner, final_out[0, :, lanes], final_in[:, lanes]))
    pair = [jnp.where(is_stator, turned(p, code, False), p) for p in pair]
    outer = [pltpu.roll(p, 4, axis=0) for p in pair]
    left = [jnp.where(is_stator, a, b) for a, b in zip(own_pair, outer)]
    right = [jnp.where(is_stator, b, a) for a, b in zip(own_pair, outer)]

    def values(pair):
        return [pair[f // 4][:, 32 * (f % 4) : 32 * (f % 4) + 32] for f in range(7)]

    diff, jump = face_parts(values(left), values(right), 2)
    sign = jnp.where(is_stator[:, :32], w, -w)
    fixes = jnp.concatenate([w * d + sign * j for d, j in zip(diff, jump)], axis=1)
    fixes = jnp.concatenate(halves(fixes), axis=0)
    tn = (((0,), (0,)), ((), ()))
    for end in range(2):
        mine = jnp.where(sub < 4 if end else sub >= 4, hot, 0.0).astype(BF16)
        spread = lax.dot_general(
            fixes, jnp.concatenate([mine, mine], axis=0), tn, preferred_element_type=F32
        )
        add_axial(end, spread)

    for f in range(5):
        for b in range(4):
            rates[f, :, 128 * b : 128 * b + 128] = acc[f, b]
    for end in range(2):
        for part in range(len(CHUNKS)):
            circ(end, part).wait_send()

    @pl.when(inner)
    def _():
        deliver().wait_send()


def on_device(mesh, radices, fields, section_store, mean_velocity, sound_speed, element_slot, face_turn, rotor_offset):
    nblk, nspan = mesh.shape["blk"], mesh.shape["span"]
    r0, r1, r2 = radices
    anywhere = pl.BlockSpec(memory_space=pltpu.HBM)
    dma = pltpu.SemaphoreType.DMA
    rates = pl.pallas_call(
        functools.partial(kernel, radices, nblk, nspan),
        out_shape=jax.ShapeDtypeStruct((5, 125, NB), F32),
        in_specs=[anywhere] * 7,
        out_specs=pl.BlockSpec(memory_space=pltpu.VMEM),
        scratch_shapes=[
            pltpu.SMEM((1, 4), I32),
            pltpu.SMEM((4,), I32),
            pltpu.VMEM((9, 4, 125, 128), F32),
            pltpu.VMEM((5, 4, 125, 128), F32),
            pltpu.VMEM((1, NB), I32),
            pltpu.VMEM((2, 3, 125, 125), BF16),
            pltpu.VMEM((NB, NB), BF16),
            pltpu.VMEM((2, PACK_ROWS, NB), F32),
            pltpu.VMEM((2, PACK_ROWS, NB), F32),
            pltpu.VMEM((2, PACK_ROWS, NB), F32),
            pltpu.VMEM((4, 256, NB), F32),
            pltpu.VMEM((4, 256, NB), F32),
            pltpu.VMEM((4, 160, NB), F32),
            pltpu.VMEM((2, 224, 128), F32),
            pltpu.VMEM((2, 224, 128), F32),
            pltpu.VMEM((8, 256), F32),
            pltpu.VMEM((r0, 8, 256), F32),
            pltpu.VMEM((16, 256), F32),
            pltpu.VMEM((r1 * r2 - 1, 16, 256), F32),
            pltpu.VMEM((2, 8, 256), F32),
            pltpu.VMEM((8, 256), F32),
            dma((10, 4)),
            dma((2, len(CHUNKS))),
            dma((2, len(CHUNKS))),
            dma((2,)),
            dma((2,)),
            dma((r0,)),
            dma((r0,)),
            dma((r1 * r2 - 1,)),
            dma((r1 * r2 - 1,)),
            pltpu.SemaphoreType.REGULAR,
        ],
        compiler_params=pltpu.CompilerParams(
            collective_id=0, has_side_effects=True, vmem_limit_bytes=40 * 2**20
        ),
        name="rates",
    )(
        *[
            pltpu.with_memory_space_constraint(value, pltpu.HBM)
            for value in (
                fields,
                mean_velocity,
                sound_speed,
                element_slot.reshape(1, NB),
                jnp.asarray(slope_matrices()),
                face_turn,
                rotor_offset,
            )
        ]
    )
    store_next = section_decay * section_store + time_step * rates
    fields_next = fields + section_gain * store_next
    return fields_next, store_next


def solution(mesh, radices=RADICES):
    both = ("blk", "span")
    in_specs = (
        P(None, None, both),
        P(None, None, both),
        P(None, None, both),
        P(None, both),
        P(both),
        P("blk", "span"),
        P("span"),
    )
    return jax.shard_map(
        functools.partial(on_device, mesh, radices),
        mesh=mesh,
        in_specs=in_specs,
        out_specs=(P(None, None, both), P(None, None, both)),
        check_vma=False,
    )
```

```python
import functools

import jax
import jax.numpy as jnp
import numpy as np
from jax import lax
from jax.experimental import pallas as pl
from jax.experimental.pallas import tpu as pltpu
from jax.sharding import PartitionSpec as P

MESH = pl.DeviceIdType.MESH
F32, BF16, I32 = jnp.float32, jnp.bfloat16, jnp.int32

section_decay = -567301805773.0 / 1357537059087.0
section_gain = 5161836677717.0 / 13612068292357.0
time_step = 0.05
metric_scale = (1.0, 1.5, 0.75)
end_weight = 0.1

NB = 512
HALF = 64
RADICES = (4, 2, 4)
CHUNKS = ((0, 32), (32, 64), (96, 56), (152, 24))
PACK_ROWS = 176
PACK_ORDER = (5, 8, 1, 4, 0, 2, 3)


def lobatto_slopes():
    root = np.sqrt(3.0 / 7.0)
    x = np.array([-1.0, -root, 0.0, root, 1.0])
    table = np.zeros((5, 5))
    for r in range(5):
        for c in range(5):
            others = [o for o in range(5) if o != r]
            if r == c:
                table[r, c] = sum(1.0 / (x[r] - x[o]) for o in others)
            else:
                top = np.prod([x[r] - x[o] for o in others])
                low = np.prod([x[c] - x[o] for o in range(5) if o != c])
                table[r, c] = top / (low * (x[r] - x[c]))
    return table


def slope_matrices():
    d, e = lobatto_slopes(), np.eye(5)
    full = [np.kron(np.kron(d, e), e), np.kron(np.kron(e, d), e), np.kron(np.kron(e, e), d)]
    full = np.stack([-time_step * g * m for g, m in zip(metric_scale, full)])
    high = full.astype(BF16)
    return np.stack([high, (full - high.astype(np.float64)).astype(BF16)])


def halves(x):
    high = x.astype(BF16)
    return high, (x - high.astype(F32)).astype(BF16)


def moved(x, table, transposed=False):
    rows = x.shape[0]
    high, low = halves(x)
    both = jnp.concatenate([high, low], axis=0)
    dims = (((1,), (1 if transposed else 0,)), ((), ()))
    out = lax.dot_general(both, table, dims, preferred_element_type=F32)
    return out[:rows] + out[rows:]


def reach_of(left, right):
    return jnp.maximum(jnp.abs(left[5]) + left[6], jnp.abs(right[5]) + right[6])


def face_value(left, right, d, reach, f):
    sides = []
    for q in (left, right):
        flux = q[5] * q[f]
        if f == 0 or f == 4:
            flux = flux + q[6] * q[1 + d]
        elif f == 1 + d:
            flux = flux + q[6] * q[4]
        sides.append(flux)
    return sides[0] - sides[1], reach * (right[f] - left[f])


def face_parts(left, right, d):
    reach = reach_of(left, right)
    return zip(*[face_value(left, right, d, reach, f) for f in range(5)])


def one_hot(row, count):
    k = lax.broadcasted_iota(I32, (count, row.shape[1]), 0).astype(F32)
    return jnp.where(k == row, 1.0, 0.0).astype(BF16)


def turned(x, code, inverse):
    lane = lax.broadcasted_iota(I32, (8, 128), 1)
    n = lane & 31
    i = (n * 13) >> 6
    k = n - i * 5
    ok = n < 25
    base = lane - n

    def apply(v, bit, target):
        index = jnp.where(ok, base + target, lane)
        return jnp.where((code & bit) != 0, jnp.take_along_axis(v, index, axis=1), v)

    swap, first, second = (4, k * 5 + i), (1, (4 - i) * 5 + k), (2, i * 5 + 4 - k)
    for bit, target in (second, first, swap) if inverse else (swap, first, second):
        x = apply(x, bit, target)
    return x


def kernel(
    radices,
    nblk,
    nspan,
    fields,
    store,
    mean,
    sound,
    slot_hbm,
    slopes_hbm,
    turn_hbm,
    offset_hbm,
    acc,
    fixed,
    turn,
    offset,
    x,
    old,
    slot,
    slopes,
    table,
    pack,
    recv,
    near,
    swaps,
    face,
    grid,
    corr,
    sp_send,
    sp_recv,
    own_packet,
    gathered,
    bundle,
    hops,
    final_out,
    final_in,
    load_sem,
    old_sem,
    circ_send,
    circ_recv,
    span_send,
    span_recv,
    hop_send,
    hop_recv,
    plane_send,
    plane_recv,
    far_sem,
):
    t = lax.axis_index("blk")
    slab = lax.axis_index("span")
    after, before = lax.rem(t + 1, nblk), lax.rem(t + nblk - 1, nblk)
    above, below = lax.rem(slab + 1, nspan), lax.rem(slab + nspan - 1, nspan)

    r0, r1, r2 = radices
    z, y, x_at = lax.rem(t, r0), lax.rem(t // r0, r1), t // (r0 * r1)
    is_first, is_last = z == 0, z == r0 - 1
    inner = jnp.logical_and(z > 0, z < r0 - 1)
    run = [t + (lax.rem(z + step, r0) - z) for step in range(1, r0)]
    across = [jnp.logical_and(z == 0, step == r0 - 1) | jnp.logical_and(z == r0 - 1, step == 1) for step in range(1, r0)]
    plane = []
    for dy in range(r1):
        for dx in range(r2):
            if dy or dx:
                to = z + r0 * lax.rem(y + dy, r1) + r0 * r1 * lax.rem(x_at + dx, r2)
                plane.append((dy, dx, to))

    barrier = pltpu.get_barrier_semaphore()
    for to in (above, below):
        pl.semaphore_signal(barrier, inc=1, device_id={"span": to}, device_id_type=MESH)
    for to, skip in zip(run, across):

        @pl.when(jnp.logical_not(skip))
        def _():
            pl.semaphore_signal(barrier, inc=1, device_id={"blk": to}, device_id_type=MESH)

    @pl.when(inner)
    def _():
        for _, _, to in plane:
            pl.semaphore_signal(barrier, inc=1, device_id={"blk": to}, device_id_type=MESH)

    @pl.when(is_first)
    def _():
        pl.semaphore_signal(barrier, inc=1, device_id={"blk": before}, device_id_type=MESH)

    def load(src):
        if src < 5:
            array = fields.at[src]
        else:
            array = mean.at[src - 5] if src < 8 else sound
        return [
            pltpu.make_async_copy(array.at[:, pl.ds(128 * b, 128)], x.at[src, b], load_sem.at[src])
            for b in range(4)
        ]

    def arrived_all(ref, sem):
        pltpu.make_async_copy(ref, ref, sem).wait()

    def loaded(src):
        arrived_all(x.at[src], load_sem.at[src])

    def cells(src, rows=slice(0, 125)):
        return jnp.concatenate([x[src, b, rows, :] for b in range(4)], axis=1)

    load_slot = pltpu.make_async_copy(slot_hbm, slot, load_sem.at[9])
    load_slopes = pltpu.make_async_copy(slopes_hbm, slopes, load_sem.at[10])
    load_turn = pltpu.make_async_copy(turn_hbm, turn, load_sem.at[11])
    load_offset = pltpu.make_async_copy(offset_hbm, offset, load_sem.at[12])
    load_slot.start()
    for src in PACK_ORDER + (7, 6):
        for copy in load(src):
            copy.start()
    load_slopes.start()
    for f in range(5):
        for b in range(4):
            pltpu.make_async_copy(
                store.at[f, :, pl.ds(128 * b, 128)], old.at[f, b], old_sem.at[f]
            ).start()
    load_turn.start()
    load_offset.start()

    load_slot.wait()
    slot_row = slot[...].astype(F32)
    for end in range(2):
        pack[end, 0:1, :] = slot_row

    def circ(end, part):
        start, rows = CHUNKS[part]
        return pltpu.make_async_remote_copy(
            src_ref=pack.at[end, pl.ds(start, rows), :],
            dst_ref=recv.at[1 - end, pl.ds(start, rows), :],
            send_sem=circ_send.at[end],
            recv_sem=circ_recv.at[1 - end, part],
            device_id={"blk": after if end == 1 else before},
            device_id_type=MESH,
        )

    def start_circ(*parts):
        for part in parts:

            @pl.when(jnp.logical_not(is_last))
            def _():
                circ(1, part).start()

            @pl.when(jnp.logical_not(is_first))
            def _():
                circ(0, part).start()

    every = range(len(CHUNKS))

    for at, src in enumerate(PACK_ORDER):
        loaded(src)
        pack[1, 1 + 25 * at : 26 + 25 * at, :] = cells(src, slice(100, 125))

    @pl.when(is_last)
    def _():
        pl.semaphore_wait(barrier, r0 + 1)
        pl.semaphore_signal(far_sem, inc=1, device_id={"blk": after}, device_id_type=MESH)
        for part in every:
            circ(1, part).start()

    lane = lax.broadcasted_iota(I32, (8, NB), 1)
    sub = lax.broadcasted_iota(I32, (8, NB), 0)
    wanted = jnp.where(sub < 4, sub * 128 + (HALF - 1), (sub - 4) * 128 + HALF)
    column = jnp.sum(jnp.where(lane == wanted, slot_row, 0.0), axis=1, keepdims=True)
    hot = jnp.where(lane.astype(F32) == column, 1.0, 0.0)

    loaded(7)
    def pack_faces(d):
        for at, src in enumerate((0, 1, 2, 3, 4, 4 + 1 + d, 8)):
            for end in range(2):
                kind = 2 * (d - 1) + end
                if d == 2:
                    face[kind, 32 * at : 32 * at + 25, :] = cells(src, pl.ds(4 * end, 25, stride=5))
                else:
                    for i in range(5):
                        rows = slice(25 * i + 20 * end, 25 * i + 20 * end + 5)
                        face[kind, 32 * at + 5 * i : 32 * at + 5 * i + 5, :] = cells(src, rows)

    pack_faces(2)
    dims = (((1,), (1,)), ((), ()))
    packet = jnp.zeros((8, 256), F32)
    for kind, rows in ((3, sub < 4), (2, sub >= 4)):
        pick = jnp.where(rows, hot, 0.0).astype(BF16)
        for part in halves(face[kind]):
            packet = packet + lax.dot_general(pick, part, dims, preferred_element_type=F32)

    sub1 = lax.broadcasted_iota(I32, (8, 128), 0)
    row = sub1 & 3
    is_stator = sub1 < 4

    def per_row(values):
        out = jnp.full((8, 128), values[3], I32)
        for s in range(3):
            out = jnp.where(row == s, values[s], out)
        return out

    load_turn.wait()
    load_offset.wait()
    code = per_row([turn[0, s] for s in range(4)])
    shift = per_row([offset[s] for s in range(4)])
    shift = jnp.where(is_stator, shift, (nblk - shift) & (nblk - 1))
    own_pair = [packet[:, :128], packet[:, 128:]]
    pair = [jnp.where(is_stator, p, turned(p, code, True)) for p in own_pair]

    for h in range(2):
        own_packet[:, 128 * h : 128 * h + 128] = pair[h]

    def collect(to_z, from_z):
        return pltpu.make_async_remote_copy(
            src_ref=own_packet,
            dst_ref=gathered.at[from_z],
            send_sem=hop_send.at[to_z],
            recv_sem=hop_recv.at[from_z],
            device_id={"blk": t + to_z - z},
            device_id_type=MESH,
        )

    @pl.when(jnp.logical_not(is_last))
    def _():
        pl.semaphore_wait(barrier, jnp.where(inner, 2 + r0 - 1 + len(plane), r0))

    for to_z in range(1, r0 - 1):

        @pl.when(z != to_z)
        def _():
            collect(to_z, z).start()

    for at, src in enumerate(PACK_ORDER):
        pack[0, 1 + 25 * at : 26 + 25 * at, :] = cells(src, slice(0, 25))
    start_circ(*every)

    table[...] = one_hot(slot_row, NB)
    loaded(6)
    pack_faces(1)

    def take_collected():
        @pl.when(inner)
        def _():
            for from_z in range(r0):

                @pl.when(z != from_z)
                def _():
                    collect(1, from_z).wait_recv()

        for to_z in range(1, r0 - 1):

            @pl.when(z != to_z)
            def _():
                collect(to_z, 0).wait_send()

        for h in range(2):
            lanes = slice(128 * h, 128 * h + 128)
            for half, target in enumerate((z, outer_z)):
                source = lax.rem(target + r0 - shift0, r0)
                value = pair[h]
                for from_z in range(r0):
                    value = jnp.where((source == from_z) & (z != from_z), gathered[from_z, :, lanes], value)
                bundle[8 * half : 8 * half + 8, lanes] = value

    outer_z = jnp.where(z == 1, 0, r0 - 1)
    shift0 = lax.rem(shift, r0)
    shift1 = lax.rem(shift // r0, r1)
    shift2 = shift // (r0 * r1)

    def hop(number):
        return pltpu.make_async_remote_copy(
            src_ref=bundle,
            dst_ref=hops.at[number],
            send_sem=plane_send.at[0],
            recv_sem=plane_recv.at[0],
            device_id={"blk": plane[number][2]},
            device_id_type=MESH,
        )

    def start_plane():
        @pl.when(inner)
        def _():
            for number in range(len(plane)):
                hop(number).start()

    def take_plane():
        @pl.when(inner)
        def _():
            arrived_all(hops, plane_send.at[0])
            arrived_all(hops, plane_recv.at[0])

        for half, target in enumerate((z, outer_z)):
            up1 = shift1 + jnp.where(target < shift0, 1, 0)
            source1 = lax.rem(y + 2 * r1 - up1, r1)
            move1 = lax.rem(up1, r1)
            move2 = lax.rem(shift2 + (source1 + up1) // r1, r2)
            for h in range(2):
                lanes = slice(128 * h, 128 * h + 128)
                rows = slice(8 * half, 8 * half + 8)
                value = bundle[rows, lanes]
                for number, (dy, dx, _) in enumerate(plane):
                    value = jnp.where((move1 == dy) & (move2 == dx), hops[number, rows, lanes], value)
                final_out[half, :, lanes] = value

    def deliver():
        return pltpu.make_async_remote_copy(
            src_ref=final_out.at[1],
            dst_ref=final_in,
            send_sem=hop_send.at[0],
            recv_sem=hop_send.at[r0 - 1],
            device_id={"blk": lax.rem(t + jnp.where(z == 1, nblk - 1, 1), nblk)},
            device_id_type=MESH,
        )

    for kind in (1, 0):
        grid[kind] = moved(face[kind], table[...])
        for f in range(7):
            sp_send[kind, 25 * f : 25 * f + 25, :] = grid[
                kind, 32 * f : 32 * f + 25, 384 * kind : 384 * kind + 128
            ]


    def span(end):
        return pltpu.make_async_remote_copy(
            src_ref=sp_send.at[end],
            dst_ref=sp_recv.at[1 - end, pl.ds(0, PACK_ROWS), :],
            send_sem=span_send.at[end],
            recv_sem=span_recv.at[1 - end],
            device_id={"span": above if end == 1 else below},
            device_id_type=MESH,
        )

    has_below, has_above = slab > 0, slab < nspan - 1

    @pl.when(has_above)
    def _():
        span(1).start()

    @pl.when(has_below)
    def _():
        span(0).start()

    for kind in (2, 3):
        grid[kind] = moved(face[kind], table[...])

    def span_sent():
        @pl.when(has_above)
        def _():
            span(1).wait_send()

        @pl.when(has_below)
        def _():
            span(0).wait_send()

    load_slopes.wait()
    velocity = (5, 6, 7)

    def volume(f):
        arrived_all(old.at[f], old_sem.at[f])
        total = None
        for d in range(3):
            fx = cells(velocity[d]) * cells(f)
            if f == 0 or f == 4:
                fx = fx + cells(8) * cells(1 + d)
            elif f == 1 + d:
                fx = fx + cells(8) * cells(4)
            high, low = halves(fx)
            for m, v in ((0, high), (0, low), (1, high)):
                part = jnp.dot(slopes[m, d], v, preferred_element_type=F32)
                total = part if total is None else total + part
        for b in range(4):
            acc[f, b] = section_decay * old[f, b] + total[:, 128 * b : 128 * b + 128]

    volume(0)
    volume(1)
    @pl.when(is_first)
    def _():
        span_sent()
        pl.semaphore_wait(far_sem, 1)
        for part in every:
            circ(0, part).start()

    take_collected()
    start_plane()

    for f in (2, 3, 4):
        volume(f)

    w = 0.5 * time_step * metric_scale[2] / end_weight
    axial = lax.broadcasted_iota(I32, (32, 128), 1)
    for s in range(4):
        cols = slice(128 * s, 128 * s + 128)
        low = [grid[2, 32 * f : 32 * f + 32, cols] for f in range(7)]
        high = [grid[3, 32 * f : 32 * f + 32, cols] for f in range(7)]
        for end in range(2):
            own, far = (high, low) if end else (low, high)
            outer = []
            for f in range(7):
                v = pltpu.roll(far[f], 127 if end else 1, axis=1)
                edge = own[f] if f >= 5 else 0.0
                outer.append(jnp.where(axial == (127 if end else 0), edge, v))
            diff, jump = face_parts(own if end else outer, outer if end else own, 2)
            slides = axial == (HALF - 1 if end else HALF)
            for f in range(5):
                value = diff[f] + jump[f] if end else diff[f] - jump[f]
                corr[2 + end, 32 * f : 32 * f + 32, cols] = jnp.where(slides, 0.0, w * value)

    def add_axial(end, values):
        for f in range(5):
            lines = pl.ds(4 * end, 25, stride=5)
            for b in range(4):
                part = values[32 * f : 32 * f + 25, 128 * b : 128 * b + 128]
                acc[f, b, lines, :] = acc[f, b, lines, :] + part

    for end in range(2):
        add_axial(end, moved(corr[2 + end], table[...], transposed=True))

    far_end = jnp.where(is_last, 1, 0)
    near_end = 1 - far_end
    weight0 = 0.5 * time_step * metric_scale[0] / end_weight

    def settle_rows(end, parts):
        start, stop = CHUNKS[parts[0]][0], sum(CHUNKS[parts[-1]])
        for part in parts:
            first, rows = CHUNKS[part]
            arrived_all(recv.at[end, pl.ds(first, rows), :], circ_recv.at[end, part])
            if part == 0:
                other = one_hot(recv[end, 0:1, :], NB)
                swap = lax.dot_general(other, table[...], dims, preferred_element_type=F32)
                swaps[end] = swap.astype(BF16)
        near[end, start:stop, :] = moved(recv[end, start:stop, :], swaps[end])

    def settle(end, fields, reach=None):
        def side(ref, src):
            at = PACK_ORDER.index(src)
            return ref[end, 1 + 25 * at : 26 + 25 * at, :]

        order = (0, 1, 2, 3, 4, 5, 8)
        own = [side(pack, src) for src in order]
        other = [side(near, src) if src != 3 or 3 in fields else None for src in order]
        if reach is None:
            reach = reach_of(own, other)
        sign = jnp.where(end == 0, weight0, -weight0)
        for f in fields:
            diff, jump = face_value(other, own, 0, reach, f)
            fixed[end, f, 0:25, :] = sign * diff - weight0 * jump
        return reach

    take_plane()

    @pl.when(inner)
    def _():
        deliver().start()

    settle_rows(near_end, (0, 1, 2, 3))
    settle(near_end, (0, 1, 2, 3, 4))
    @pl.when(has_above)
    def _():
        span(0).wait_recv()

    @pl.when(has_below)
    def _():
        span(1).wait_recv()

    w = 0.5 * time_step * metric_scale[1] / end_weight
    for b in range(5):
        left, right = [], []
        for f in range(7):
            rows = slice(32 * f, 32 * f + 32)
            if b > 0:
                left.append(grid[1, rows, 128 * b - 128 : 128 * b])
            if b < 4:
                right.append(grid[0, rows, 128 * b : 128 * b + 128])
        for f in range(7):
            rows = slice(32 * f, 32 * f + 32)
            if b == 0:
                wall = -right[f] if f == 2 else right[f]
                left.append(jnp.where(has_below, sp_recv[0, 25 * f : 25 * f + 32, :], wall))
            if b == 4:
                wall = -left[f] if f == 2 else left[f]
                right.append(jnp.where(has_above, sp_recv[1, 25 * f : 25 * f + 32, :], wall))
        diff, jump = face_parts(left, right, 1)
        for f in range(5):
            if b > 0:
                corr[1, 32 * f : 32 * f + 32, 128 * b - 128 : 128 * b] = w * (diff[f] + jump[f])
            if b < 4:
                corr[0, 32 * f : 32 * f + 32, 128 * b : 128 * b + 128] = w * (diff[f] - jump[f])

    for end in range(2):
        back = moved(corr[end], table[...], transposed=True)
        for f in range(5):
            for i in range(5):
                rows = slice(25 * i + 20 * end, 25 * i + 20 * end + 5)
                for b in range(4):
                    part = back[32 * f + 5 * i : 32 * f + 5 * i + 5, 128 * b : 128 * b + 128]
                    acc[f, b, rows, :] += part
    settle_rows(far_end, (0, 1))
    settle_rows(far_end, (2,))
    reach = settle(far_end, (0, 1, 2, 4))
    settle_rows(far_end, (3,))
    settle(far_end, (3,), reach)
    @pl.when(jnp.logical_not(inner))
    def _():
        deliver().wait_recv()

    pair = []
    for h in range(2):
        lanes = slice(128 * h, 128 * h + 128)
        pair.append(jnp.where(inner, final_out[0, :, lanes], final_in[:, lanes]))
    pair = [jnp.where(is_stator, turned(p, code, False), p) for p in pair]
    outer = [pltpu.roll(p, 4, axis=0) for p in pair]
    left = [jnp.where(is_stator, a, b) for a, b in zip(own_pair, outer)]
    right = [jnp.where(is_stator, b, a) for a, b in zip(own_pair, outer)]

    def values(pair):
        return [pair[f // 4][:, 32 * (f % 4) : 32 * (f % 4) + 32] for f in range(7)]

    w = 0.5 * time_step * metric_scale[2] / end_weight
    diff, jump = face_parts(values(left), values(right), 2)
    sign = jnp.where(is_stator[:, :32], w, -w)
    fixes = jnp.concatenate([w * d + sign * j for d, j in zip(diff, jump)], axis=1)
    fixes = jnp.concatenate(halves(fixes), axis=0)
    tn = (((0,), (0,)), ((), ()))
    for end in range(2):
        mine = jnp.where(sub < 4 if end else sub >= 4, hot, 0.0).astype(BF16)
        spread = lax.dot_general(
            fixes, jnp.concatenate([mine, mine], axis=0), tn, preferred_element_type=F32
        )
        add_axial(end, spread)

    @pl.when(jnp.logical_not(is_first))
    def _():
        span_sent()

    for end in range(2):
        arrived_all(pack.at[end], circ_send.at[end])

    @pl.when(inner)
    def _():
        deliver().wait_send()


def update(partial_store, end_parts, fields, fields_next, store_next, ready, sent):
    copies = []
    for f in range(5):
        for b in range(4):
            cols = slice(128 * b, 128 * b + 128)
            for start, stop, end in ((0, 25, 0), (25, 100, None), (100, 125, 1)):
                rows = slice(start, stop)
                value = partial_store[f, b, rows, :]
                if end is not None:
                    value = value + end_parts[end, f, 0:25, cols]
                ready[1, f, rows, cols] = value
                ready[0, f, rows, cols] = fields[f, rows, cols] + section_gain * value
        for which, result in ((1, store_next), (0, fields_next)):
            copies.append(pltpu.make_async_copy(ready.at[which, f], result.at[f], sent.at[which, f]))
            copies[-1].start()
    for copy in copies:
        copy.wait()


def on_device(mesh, radices, fields, section_store, mean_velocity, sound_speed, element_slot, face_turn, rotor_offset):
    nblk, nspan = mesh.shape["blk"], mesh.shape["span"]
    r0, r1, r2 = radices
    anywhere = pl.BlockSpec(memory_space=pltpu.HBM)
    vmem = pl.BlockSpec(memory_space=pltpu.VMEM)
    dma = pltpu.SemaphoreType.DMA
    partial_store, end_parts = pl.pallas_call(
        functools.partial(kernel, radices, nblk, nspan),
        out_shape=(
            jax.ShapeDtypeStruct((5, 4, 125, 128), F32),
            jax.ShapeDtypeStruct((2, 5, 32, NB), F32),
        ),
        in_specs=[anywhere] * 8,
        out_specs=(vmem, vmem),
        scratch_shapes=[
            pltpu.SMEM((1, 4), I32),
            pltpu.SMEM((4,), I32),
            pltpu.VMEM((9, 4, 125, 128), F32),
            pltpu.VMEM((5, 4, 125, 128), F32),
            pltpu.VMEM((1, NB), I32),
            pltpu.VMEM((2, 3, 125, 125), BF16),
            pltpu.VMEM((NB, NB), BF16),
            pltpu.VMEM((2, PACK_ROWS, NB), F32),
            pltpu.VMEM((2, PACK_ROWS, NB), F32),
            pltpu.VMEM((2, PACK_ROWS, NB), F32),
            pltpu.VMEM((2, NB, NB), BF16),
            pltpu.VMEM((4, 256, NB), F32),
            pltpu.VMEM((4, 256, NB), F32),
            pltpu.VMEM((4, 160, NB), F32),
            pltpu.VMEM((2, PACK_ROWS, 128), F32),
            pltpu.VMEM((2, 184, 128), F32),
            pltpu.VMEM((8, 256), F32),
            pltpu.VMEM((r0, 8, 256), F32),
            pltpu.VMEM((16, 256), F32),
            pltpu.VMEM((r1 * r2 - 1, 16, 256), F32),
            pltpu.VMEM((2, 8, 256), F32),
            pltpu.VMEM((8, 256), F32),
            dma((13,)),
            dma((5,)),
            dma((2,)),
            dma((2, len(CHUNKS))),
            dma((2,)),
            dma((2,)),
            dma((r0,)),
            dma((r0,)),
            dma((1,)),
            dma((1,)),
            pltpu.SemaphoreType.REGULAR,
        ],
        compiler_params=pltpu.CompilerParams(
            collective_id=0, has_side_effects=True, vmem_limit_bytes=22 * 2**20
        ),
        name="rates",
    )(
        *[
            pltpu.with_memory_space_constraint(value, pltpu.HBM)
            for value in (
                fields,
                section_store,
                mean_velocity,
                sound_speed,
                element_slot.reshape(1, NB),
                jnp.asarray(slope_matrices()),
                face_turn,
                rotor_offset,
            )
        ]
    )
    whole = jax.ShapeDtypeStruct((5, 125, NB), F32)
    fields_next, store_next = pl.pallas_call(
        update,
        out_shape=(whole, whole),
        in_specs=[vmem] * 3,
        out_specs=(anywhere, anywhere),
        scratch_shapes=[
            pltpu.VMEM((2, 5, 125, NB), F32),
            dma((2, 5)),
        ],
        compiler_params=pltpu.CompilerParams(vmem_limit_bytes=12 * 2**20),
        name="update",
    )(partial_store, end_parts, fields)
    return fields_next, store_next


def solution(mesh, radices=RADICES):
    both = ("blk", "span")
    in_specs = (
        P(None, None, both),
        P(None, None, both),
        P(None, None, both),
        P(None, both),
        P(both),
        P("blk", "span"),
        P("span"),
    )
    return jax.shard_map(
        functools.partial(on_device, mesh, radices),
        mesh=mesh,
        in_specs=in_specs,
        out_specs=(P(None, None, both), P(None, None, both)),
        check_vma=False,
    )
```

```python
import functools

import jax
import jax.numpy as jnp
import numpy as np
from jax import lax
from jax.experimental import pallas as pl
from jax.experimental.pallas import tpu as pltpu
from jax.sharding import PartitionSpec as P

MESH = pl.DeviceIdType.MESH
F32, BF16, I32 = jnp.float32, jnp.bfloat16, jnp.int32

section_decay = -567301805773.0 / 1357537059087.0
section_gain = 5161836677717.0 / 13612068292357.0
time_step = 0.05
metric_scale = (1.0, 1.5, 0.75)
end_weight = 0.1

NB = 512
HALF = 64
RADICES = (4, 2, 4)
CHUNKS = ((0, 32), (32, 64), (96, 56), (152, 24))
PACK_ROWS = 176
PACK_ORDER = (5, 8, 1, 4, 0, 2, 3)


def lobatto_slopes():
    root = np.sqrt(3.0 / 7.0)
    x = np.array([-1.0, -root, 0.0, root, 1.0])
    table = np.zeros((5, 5))
    for r in range(5):
        for c in range(5):
            others = [o for o in range(5) if o != r]
            if r == c:
                table[r, c] = sum(1.0 / (x[r] - x[o]) for o in others)
            else:
                top = np.prod([x[r] - x[o] for o in others])
                low = np.prod([x[c] - x[o] for o in range(5) if o != c])
                table[r, c] = top / (low * (x[r] - x[c]))
    return table


def slope_matrices():
    d, e = lobatto_slopes(), np.eye(5)
    full = [np.kron(np.kron(d, e), e), np.kron(np.kron(e, d), e), np.kron(np.kron(e, e), d)]
    full = np.stack([-time_step * g * m for g, m in zip(metric_scale, full)])
    high = full.astype(BF16)
    return np.stack([high, (full - high.astype(np.float64)).astype(BF16)])


def halves(x):
    high = x.astype(BF16)
    return high, (x - high.astype(F32)).astype(BF16)


def moved(x, table, transposed=False):
    rows = x.shape[0]
    high, low = halves(x)
    both = jnp.concatenate([high, low], axis=0)
    dims = (((1,), (1 if transposed else 0,)), ((), ()))
    out = lax.dot_general(both, table, dims, preferred_element_type=F32)
    return out[:rows] + out[rows:]


def reach_of(left, right):
    return jnp.maximum(jnp.abs(left[5]) + left[6], jnp.abs(right[5]) + right[6])


def face_value(left, right, d, reach, f):
    sides = []
    for q in (left, right):
        flux = q[5] * q[f]
        if f == 0 or f == 4:
            flux = flux + q[6] * q[1 + d]
        elif f == 1 + d:
            flux = flux + q[6] * q[4]
        sides.append(flux)
    return sides[0] - sides[1], reach * (right[f] - left[f])


def face_parts(left, right, d):
    reach = reach_of(left, right)
    return zip(*[face_value(left, right, d, reach, f) for f in range(5)])


def one_hot(row, count):
    k = lax.broadcasted_iota(I32, (count, row.shape[1]), 0).astype(F32)
    return jnp.where(k == row, 1.0, 0.0).astype(BF16)


def turned(x, code, inverse):
    lane = lax.broadcasted_iota(I32, (8, 128), 1)
    n = lane & 31
    row = (n * 13) >> 6
    ok = n < 25
    maps = {4: lambda i, k: (k, i), 1: lambda i, k: (4 - i, k), 2: lambda i, k: (i, 4 - k)}
    result = x
    for value in range(1, 8):
        i, k = row, n - row * 5
        for bit in (4, 1, 2) if inverse else (2, 1, 4):
            if value & bit:
                i, k = maps[bit](i, k)
        index = jnp.where(ok, lane - n + i * 5 + k, lane)
        result = jnp.where(code == value, jnp.take_along_axis(x, index, axis=1), result)
    return result


def kernel(
    radices,
    nblk,
    nspan,
    fields,
    store,
    mean,
    sound,
    slot_hbm,
    slopes_hbm,
    turn_hbm,
    offset_hbm,
    acc,
    fixed,
    turn,
    offset,
    x,
    old,
    slot,
    slopes,
    table,
    pack,
    recv,
    near,
    swaps,
    hot_columns,
    face,
    grid,
    corr,
    sp_send,
    sp_recv,
    own_packet,
    gathered,
    bundle,
    hops,
    final_out,
    final_in,
    load_sem,
    old_sem,
    circ_send,
    circ_recv,
    span_send,
    span_recv,
    hop_send,
    hop_recv,
    plane_send,
    plane_recv,
    far_sem,
):
    t = lax.axis_index("blk")
    slab = lax.axis_index("span")
    after, before = lax.rem(t + 1, nblk), lax.rem(t + nblk - 1, nblk)
    above, below = lax.rem(slab + 1, nspan), lax.rem(slab + nspan - 1, nspan)

    r0, r1, r2 = radices
    z, y, x_at = lax.rem(t, r0), lax.rem(t // r0, r1), t // (r0 * r1)
    is_first, is_last = z == 0, z == r0 - 1
    inner = jnp.logical_and(z > 0, z < r0 - 1)
    run = [t + (lax.rem(z + step, r0) - z) for step in range(1, r0)]
    across = [jnp.logical_and(z == 0, step == r0 - 1) | jnp.logical_and(z == r0 - 1, step == 1) for step in range(1, r0)]
    plane = []
    for dy in range(r1):
        for dx in range(r2):
            if dy or dx:
                to = z + r0 * lax.rem(y + dy, r1) + r0 * r1 * lax.rem(x_at + dx, r2)
                plane.append((dy, dx, to))

    barrier = pltpu.get_barrier_semaphore()
    for to in (above, below):
        pl.semaphore_signal(barrier, inc=1, device_id={"span": to}, device_id_type=MESH)
    for to, skip in zip(run, across):

        @pl.when(jnp.logical_not(skip))
        def _():
            pl.semaphore_signal(barrier, inc=1, device_id={"blk": to}, device_id_type=MESH)

    @pl.when(inner)
    def _():
        for _, _, to in plane:
            pl.semaphore_signal(barrier, inc=1, device_id={"blk": to}, device_id_type=MESH)

    @pl.when(is_first)
    def _():
        pl.semaphore_signal(barrier, inc=1, device_id={"blk": before}, device_id_type=MESH)

    def load(src):
        if src < 5:
            array = fields.at[src]
        else:
            array = mean.at[src - 5] if src < 8 else sound
        return [
            pltpu.make_async_copy(array.at[:, pl.ds(128 * b, 128)], x.at[src, b], load_sem.at[src])
            for b in range(4)
        ]

    def arrived_all(ref, sem):
        pltpu.make_async_copy(ref, ref, sem).wait()

    def loaded(src):
        arrived_all(x.at[src], load_sem.at[src])

    def cells(src, rows=slice(0, 125)):
        return jnp.concatenate([x[src, b, rows, :] for b in range(4)], axis=1)

    load_slot = pltpu.make_async_copy(slot_hbm, slot, load_sem.at[9])
    load_slopes = pltpu.make_async_copy(slopes_hbm, slopes, load_sem.at[10])
    load_turn = pltpu.make_async_copy(turn_hbm, turn, load_sem.at[11])
    load_offset = pltpu.make_async_copy(offset_hbm, offset, load_sem.at[12])
    load_slot.start()
    for src in PACK_ORDER + (7, 6):
        for copy in load(src):
            copy.start()
    load_slopes.start()
    for f in range(5):
        for b in range(4):
            pltpu.make_async_copy(
                store.at[f, :, pl.ds(128 * b, 128)], old.at[f, b], old_sem.at[0]
            ).start()
    load_turn.start()
    load_offset.start()

    load_slot.wait()
    slot_row = slot[...].astype(F32)
    for end in range(2):
        pack[end, 0:1, :] = slot_row

    def circ(end, part):
        start, rows = CHUNKS[part]
        return pltpu.make_async_remote_copy(
            src_ref=pack.at[end, pl.ds(start, rows), :],
            dst_ref=recv.at[1 - end, pl.ds(start, rows), :],
            send_sem=circ_send.at[end],
            recv_sem=circ_recv.at[1 - end, part],
            device_id={"blk": after if end == 1 else before},
            device_id_type=MESH,
        )

    def start_circ(*parts):
        for part in parts:

            @pl.when(jnp.logical_not(is_last))
            def _():
                circ(1, part).start()

            @pl.when(jnp.logical_not(is_first))
            def _():
                circ(0, part).start()

    every = range(len(CHUNKS))

    lane = lax.broadcasted_iota(I32, (8, NB), 1)
    sub = lax.broadcasted_iota(I32, (8, NB), 0)
    wanted = jnp.where(sub < 4, sub * 128 + (HALF - 1), (sub - 4) * 128 + HALF)
    column = jnp.sum(jnp.where(lane == wanted, slot_row, 0.0), axis=1, keepdims=True)
    hot = jnp.where(lane.astype(F32) == column, 1.0, 0.0)
    wide = jnp.concatenate([hot, jnp.zeros((120, NB), F32)], axis=0)
    hot_columns[...] = jnp.transpose(wide).astype(BF16)

    def far_start(*parts):
        @pl.when(is_last)
        def _():
            if parts[0] == 0:
                pl.semaphore_wait(barrier, r0 + 1)
                pl.semaphore_signal(far_sem, inc=1, device_id={"blk": after}, device_id_type=MESH)
            for part in parts:
                circ(1, part).start()

    for at, src in enumerate(PACK_ORDER):
        loaded(src)
        pack[1, 1 + 25 * at : 26 + 25 * at, :] = cells(src, slice(100, 125))
        if at == 1:
            far_start(0)
        if at == 3:
            far_start(1)
    far_start(2, 3)

    loaded(7)
    def pack_faces(d):
        for at, src in enumerate((0, 1, 2, 3, 4, 4 + 1 + d, 8)):
            for end in range(2):
                kind = 2 * (d - 1) + end
                if d == 2:
                    face[kind, 32 * at : 32 * at + 25, :] = cells(src, pl.ds(4 * end, 25, stride=5))
                else:
                    for i in range(5):
                        rows = slice(25 * i + 20 * end, 25 * i + 20 * end + 5)
                        face[kind, 32 * at + 5 * i : 32 * at + 5 * i + 5, :] = cells(src, rows)

    pack_faces(2)
    dims = (((1,), (1,)), ((), ()))
    picked = []
    for kind in (3, 2):
        both = jnp.concatenate(halves(face[kind]), axis=0)
        part = jnp.dot(both, hot_columns[...], preferred_element_type=F32)
        picked.append(part[:256] + part[256:])
    stator_lane = lax.broadcasted_iota(I32, (256, 128), 1) < 4
    packet = jnp.transpose(jnp.where(stator_lane, picked[0], picked[1]))[:8]

    sub1 = lax.broadcasted_iota(I32, (8, 128), 0)
    row = sub1 & 3
    is_stator = sub1 < 4

    def per_row(values):
        out = jnp.full((8, 128), values[3], I32)
        for s in range(3):
            out = jnp.where(row == s, values[s], out)
        return out

    load_turn.wait()
    load_offset.wait()
    code = per_row([turn[0, s] for s in range(4)])
    shift = per_row([offset[s] for s in range(4)])
    shift = jnp.where(is_stator, shift, (nblk - shift) & (nblk - 1))
    own_pair = [packet[:, :128], packet[:, 128:]]
    pair = [jnp.where(is_stator, p, turned(p, code, True)) for p in own_pair]

    for h in range(2):
        own_packet[:, 128 * h : 128 * h + 128] = pair[h]

    def collect(to_z, from_z):
        return pltpu.make_async_remote_copy(
            src_ref=own_packet,
            dst_ref=gathered.at[from_z],
            send_sem=hop_send.at[to_z],
            recv_sem=hop_recv.at[0],
            device_id={"blk": t + to_z - z},
            device_id_type=MESH,
        )

    @pl.when(jnp.logical_not(is_last))
    def _():
        pl.semaphore_wait(barrier, jnp.where(inner, 2 + r0 - 1 + len(plane), r0))

    for to_z in range(1, r0 - 1):

        @pl.when(z != to_z)
        def _():
            collect(to_z, z).start()

    for at, src in enumerate(PACK_ORDER):
        pack[0, 1 + 25 * at : 26 + 25 * at, :] = cells(src, slice(0, 25))
    start_circ(*every)

    table[...] = one_hot(slot_row, NB)
    loaded(6)
    pack_faces(1)

    def take_collected():
        @pl.when(inner)
        def _():
            arrived_all(gathered.at[pl.ds(0, r0 - 1)], hop_recv.at[0])

        for to_z in range(1, r0 - 1):

            @pl.when(z != to_z)
            def _():
                collect(to_z, 0).wait_send()

        for h in range(2):
            lanes = slice(128 * h, 128 * h + 128)
            for half, target in enumerate((z, outer_z)):
                source = lax.rem(target + r0 - shift0, r0)
                value = pair[h]
                for from_z in range(r0):
                    value = jnp.where((source == from_z) & (z != from_z), gathered[from_z, :, lanes], value)
                bundle[8 * half : 8 * half + 8, lanes] = value

    outer_z = jnp.where(z == 1, 0, r0 - 1)
    shift0 = lax.rem(shift, r0)
    shift1 = lax.rem(shift // r0, r1)
    shift2 = shift // (r0 * r1)

    def hop(number):
        return pltpu.make_async_remote_copy(
            src_ref=bundle,
            dst_ref=hops.at[number],
            send_sem=plane_send.at[0],
            recv_sem=plane_recv.at[0],
            device_id={"blk": plane[number][2]},
            device_id_type=MESH,
        )

    def start_plane():
        @pl.when(inner)
        def _():
            for number in range(len(plane)):
                hop(number).start()

    def take_plane():
        @pl.when(inner)
        def _():
            arrived_all(hops, plane_send.at[0])
            arrived_all(hops, plane_recv.at[0])

        for half, target in enumerate((z, outer_z)):
            up1 = shift1 + jnp.where(target < shift0, 1, 0)
            source1 = lax.rem(y + 2 * r1 - up1, r1)
            move1 = lax.rem(up1, r1)
            move2 = lax.rem(shift2 + (source1 + up1) // r1, r2)
            for h in range(2):
                lanes = slice(128 * h, 128 * h + 128)
                rows = slice(8 * half, 8 * half + 8)
                value = bundle[rows, lanes]
                for number, (dy, dx, _) in enumerate(plane):
                    value = jnp.where((move1 == dy) & (move2 == dx), hops[number, rows, lanes], value)
                final_out[half, :, lanes] = value

    def deliver():
        return pltpu.make_async_remote_copy(
            src_ref=final_out.at[1],
            dst_ref=final_in,
            send_sem=hop_send.at[0],
            recv_sem=hop_send.at[r0 - 1],
            device_id={"blk": lax.rem(t + jnp.where(z == 1, nblk - 1, 1), nblk)},
            device_id_type=MESH,
        )

    for kind in (1, 0):
        grid[kind] = moved(face[kind], table[...])
        for f in range(7):
            sp_send[kind, 25 * f : 25 * f + 25, :] = grid[
                kind, 32 * f : 32 * f + 25, 384 * kind : 384 * kind + 128
            ]


    def span(end):
        return pltpu.make_async_remote_copy(
            src_ref=sp_send.at[end],
            dst_ref=sp_recv.at[1 - end, pl.ds(0, PACK_ROWS), :],
            send_sem=span_send.at[end],
            recv_sem=span_recv.at[1 - end],
            device_id={"span": above if end == 1 else below},
            device_id_type=MESH,
        )

    has_below, has_above = slab > 0, slab < nspan - 1

    def start_span(when):
        @pl.when(jnp.logical_and(when, has_above))
        def _():
            span(1).start()

        @pl.when(jnp.logical_and(when, has_below))
        def _():
            span(0).start()

    start_span(jnp.logical_not(is_last))

    for kind in (2, 3):
        grid[kind] = moved(face[kind], table[...])

    def span_sent():
        @pl.when(has_above)
        def _():
            span(1).wait_send()

        @pl.when(has_below)
        def _():
            span(0).wait_send()

    load_slopes.wait()
    velocity = (5, 6, 7)

    arrived_all(old, old_sem.at[0])

    def volume(f):
        total = None
        for d in range(3):
            fx = cells(velocity[d]) * cells(f)
            if f == 0 or f == 4:
                fx = fx + cells(8) * cells(1 + d)
            elif f == 1 + d:
                fx = fx + cells(8) * cells(4)
            high, low = halves(fx)
            for m, v in ((0, high), (0, low), (1, high)):
                part = jnp.dot(slopes[m, d], v, preferred_element_type=F32)
                total = part if total is None else total + part
        for b in range(4):
            acc[f, b] = section_decay * old[f, b] + total[:, 128 * b : 128 * b + 128]

    volume(0)
    volume(1)
    @pl.when(is_first)
    def _():
        span_sent()
        pl.semaphore_wait(far_sem, 1)
        for part in every:
            circ(0, part).start()

    take_collected()
    start_plane()

    for f in (2, 3, 4):
        volume(f)

    w = 0.5 * time_step * metric_scale[2] / end_weight
    axial = lax.broadcasted_iota(I32, (32, 128), 1)
    for s in range(4):
        cols = slice(128 * s, 128 * s + 128)
        low = [grid[2, 32 * f : 32 * f + 32, cols] for f in range(7)]
        high = [grid[3, 32 * f : 32 * f + 32, cols] for f in range(7)]
        for end in range(2):
            own, far = (high, low) if end else (low, high)
            outer = []
            for f in range(7):
                v = pltpu.roll(far[f], 127 if end else 1, axis=1)
                edge = own[f] if f >= 5 else 0.0
                outer.append(jnp.where(axial == (127 if end else 0), edge, v))
            diff, jump = face_parts(own if end else outer, outer if end else own, 2)
            slides = axial == (HALF - 1 if end else HALF)
            for f in range(5):
                value = diff[f] + jump[f] if end else diff[f] - jump[f]
                corr[2 + end, 32 * f : 32 * f + 32, cols] = jnp.where(slides, 0.0, w * value)

    def add_axial(end, values):
        for f in range(5):
            lines = pl.ds(4 * end, 25, stride=5)
            for b in range(4):
                part = values[32 * f : 32 * f + 25, 128 * b : 128 * b + 128]
                acc[f, b, lines, :] = acc[f, b, lines, :] + part

    for end in range(2):
        add_axial(end, moved(corr[2 + end], table[...], transposed=True))

    far_end = jnp.where(is_last, 1, 0)
    near_end = 1 - far_end
    weight0 = 0.5 * time_step * metric_scale[0] / end_weight

    def settle_rows(end, parts):
        start, stop = CHUNKS[parts[0]][0], sum(CHUNKS[parts[-1]])
        for part in parts:
            first, rows = CHUNKS[part]
            arrived_all(recv.at[end, pl.ds(first, rows), :], circ_recv.at[end, part])
            if part == 0:
                other = one_hot(recv[end, 0:1, :], NB)
                swap = lax.dot_general(other, table[...], dims, preferred_element_type=F32)
                swaps[end] = swap.astype(BF16)
        near[end, start:stop, :] = moved(recv[end, start:stop, :], swaps[end])

    def settle(end, fields, reach=None):
        def side(ref, src):
            at = PACK_ORDER.index(src)
            return ref[end, 1 + 25 * at : 26 + 25 * at, :]

        order = (0, 1, 2, 3, 4, 5, 8)
        own = [side(pack, src) for src in order]
        other = [side(near, src) if src != 3 or 3 in fields else None for src in order]
        if reach is None:
            reach = reach_of(own, other)
        sign = jnp.where(end == 0, weight0, -weight0)
        for f in fields:
            diff, jump = face_value(other, own, 0, reach, f)
            fixed[end, f, 0:25, :] = sign * diff - weight0 * jump
        return reach

    @pl.when(is_last)
    def _():
        arrived_all(pack.at[1], circ_send.at[1])

    start_span(is_last)
    @pl.when(has_above)
    def _():
        span(0).wait_recv()

    @pl.when(has_below)
    def _():
        span(1).wait_recv()

    w = 0.5 * time_step * metric_scale[1] / end_weight
    for b in range(5):
        left, right = [], []
        for f in range(7):
            rows = slice(32 * f, 32 * f + 32)
            if b > 0:
                left.append(grid[1, rows, 128 * b - 128 : 128 * b])
            if b < 4:
                right.append(grid[0, rows, 128 * b : 128 * b + 128])
        for f in range(7):
            rows = slice(32 * f, 32 * f + 32)
            if b == 0:
                wall = -right[f] if f == 2 else right[f]
                left.append(jnp.where(has_below, sp_recv[0, 25 * f : 25 * f + 32, :], wall))
            if b == 4:
                wall = -left[f] if f == 2 else left[f]
                right.append(jnp.where(has_above, sp_recv[1, 25 * f : 25 * f + 32, :], wall))
        diff, jump = face_parts(left, right, 1)
        for f in range(5):
            if b > 0:
                corr[1, 32 * f : 32 * f + 32, 128 * b - 128 : 128 * b] = w * (diff[f] + jump[f])
            if b < 4:
                corr[0, 32 * f : 32 * f + 32, 128 * b : 128 * b + 128] = w * (diff[f] - jump[f])

    for end in range(2):
        back = moved(corr[end], table[...], transposed=True)
        for f in range(5):
            for i in range(5):
                rows = slice(25 * i + 20 * end, 25 * i + 20 * end + 5)
                for b in range(4):
                    part = back[32 * f + 5 * i : 32 * f + 5 * i + 5, 128 * b : 128 * b + 128]
                    acc[f, b, rows, :] += part
    take_plane()

    @pl.when(inner)
    def _():
        deliver().start()

    settle_rows(near_end, (0, 1, 2, 3))
    settle(near_end, (0, 1, 2, 3, 4))
    settle_rows(far_end, (0, 1))
    def slide():
        @pl.when(jnp.logical_not(inner))
        def _():
            deliver().wait_recv()

        pair = []
        for h in range(2):
            lanes = slice(128 * h, 128 * h + 128)
            pair.append(jnp.where(inner, final_out[0, :, lanes], final_in[:, lanes]))
        pair = [jnp.where(is_stator, turned(p, code, False), p) for p in pair]
        outer = [pltpu.roll(p, 4, axis=0) for p in pair]
        left = [jnp.where(is_stator, a, b) for a, b in zip(own_pair, outer)]
        right = [jnp.where(is_stator, b, a) for a, b in zip(own_pair, outer)]

        def values(pair):
            return [pair[f // 4][:, 32 * (f % 4) : 32 * (f % 4) + 32] for f in range(7)]

        w = 0.5 * time_step * metric_scale[2] / end_weight
        diff, jump = face_parts(values(left), values(right), 2)
        sign = jnp.where(is_stator[:, :32], w, -w)
        fixes = jnp.concatenate([w * d + sign * j for d, j in zip(diff, jump)], axis=1)
        fixes = jnp.concatenate(halves(fixes), axis=0)
        tn = (((0,), (0,)), ((), ()))
        spots = jnp.concatenate([jnp.where(sub >= 4, hot, 0.0), jnp.where(sub < 4, hot, 0.0)], axis=1)
        spots = jnp.concatenate([spots, spots], axis=0).astype(BF16)
        spread = lax.dot_general(fixes, spots, tn, preferred_element_type=F32)
        for end in range(2):
            add_axial(end, spread[:, NB * end : NB * end + NB])

    second = lax.rem(slab, 2) == 1
    pl.when(second)(slide)
    settle_rows(far_end, (2,))
    reach = settle(far_end, (0, 1, 2, 4))
    settle_rows(far_end, (3,))
    settle(far_end, (3,), reach)
    pl.when(jnp.logical_not(second))(slide)
    @pl.when(jnp.logical_not(is_first))
    def _():
        span_sent()

    arrived_all(pack.at[0], circ_send.at[0])

    @pl.when(jnp.logical_not(is_last))
    def _():
        arrived_all(pack.at[1], circ_send.at[1])


    @pl.when(inner)
    def _():
        deliver().wait_send()


def update(partial_store, end_parts, fields, fields_next, store_next, ready, sent):
    copies = []
    for f in range(5):
        for b in range(4):
            cols = slice(128 * b, 128 * b + 128)
            for start, stop, end in ((0, 25, 0), (25, 100, None), (100, 125, 1)):
                rows = slice(start, stop)
                value = partial_store[f, b, rows, :]
                if end is not None:
                    value = value + end_parts[end, f, 0:25, cols]
                ready[1, f, rows, cols] = value
                ready[0, f, rows, cols] = fields[f, rows, cols] + section_gain * value
        for which, result in ((1, store_next), (0, fields_next)):
            copies.append(pltpu.make_async_copy(ready.at[which, f], result.at[f], sent.at[which, f]))
            copies[-1].start()
    for copy in copies:
        copy.wait()


def on_device(mesh, radices, fields, section_store, mean_velocity, sound_speed, element_slot, face_turn, rotor_offset):
    nblk, nspan = mesh.shape["blk"], mesh.shape["span"]
    r0, r1, r2 = radices
    anywhere = pl.BlockSpec(memory_space=pltpu.HBM)
    vmem = pl.BlockSpec(memory_space=pltpu.VMEM)
    dma = pltpu.SemaphoreType.DMA
    partial_store, end_parts = pl.pallas_call(
        functools.partial(kernel, radices, nblk, nspan),
        out_shape=(
            jax.ShapeDtypeStruct((5, 4, 125, 128), F32),
            jax.ShapeDtypeStruct((2, 5, 32, NB), F32),
        ),
        in_specs=[anywhere] * 8,
        out_specs=(vmem, vmem),
        scratch_shapes=[
            pltpu.SMEM((1, 4), I32),
            pltpu.SMEM((4,), I32),
            pltpu.VMEM((9, 4, 125, 128), F32),
            pltpu.VMEM((5, 4, 125, 128), F32),
            pltpu.VMEM((1, NB), I32),
            pltpu.VMEM((2, 3, 125, 125), BF16),
            pltpu.VMEM((NB, NB), BF16),
            pltpu.VMEM((2, PACK_ROWS, NB), F32),
            pltpu.VMEM((2, PACK_ROWS, NB), F32),
            pltpu.VMEM((2, PACK_ROWS, NB), F32),
            pltpu.VMEM((2, NB, NB), BF16),
            pltpu.VMEM((NB, 128), BF16),
            pltpu.VMEM((4, 256, NB), F32),
            pltpu.VMEM((4, 256, NB), F32),
            pltpu.VMEM((4, 160, NB), F32),
            pltpu.VMEM((2, PACK_ROWS, 128), F32),
            pltpu.VMEM((2, 184, 128), F32),
            pltpu.VMEM((8, 256), F32),
            pltpu.VMEM((r0, 8, 256), F32),
            pltpu.VMEM((16, 256), F32),
            pltpu.VMEM((r1 * r2 - 1, 16, 256), F32),
            pltpu.VMEM((2, 8, 256), F32),
            pltpu.VMEM((8, 256), F32),
            dma((13,)),
            dma((1,)),
            dma((2,)),
            dma((2, len(CHUNKS))),
            dma((2,)),
            dma((2,)),
            dma((r0,)),
            dma((1,)),
            dma((1,)),
            dma((1,)),
            pltpu.SemaphoreType.REGULAR,
        ],
        compiler_params=pltpu.CompilerParams(
            collective_id=0, has_side_effects=True, vmem_limit_bytes=22 * 2**20
        ),
        name="rates",
    )(
        *[
            pltpu.with_memory_space_constraint(value, pltpu.HBM)
            for value in (
                fields,
                section_store,
                mean_velocity,
                sound_speed,
                element_slot.reshape(1, NB),
                jnp.asarray(slope_matrices()),
                face_turn,
                rotor_offset,
            )
        ]
    )
    whole = jax.ShapeDtypeStruct((5, 125, NB), F32)
    fields_next, store_next = pl.pallas_call(
        update,
        out_shape=(whole, whole),
        in_specs=[vmem] * 3,
        out_specs=(anywhere, anywhere),
        scratch_shapes=[
            pltpu.VMEM((2, 5, 125, NB), F32),
            dma((2, 5)),
        ],
        compiler_params=pltpu.CompilerParams(vmem_limit_bytes=12 * 2**20),
        name="update",
    )(partial_store, end_parts, fields)
    return fields_next, store_next


def solution(mesh, radices=RADICES):
    both = ("blk", "span")
    in_specs = (
        P(None, None, both),
        P(None, None, both),
        P(None, None, both),
        P(None, both),
        P(both),
        P("blk", "span"),
        P("span"),
    )
    return jax.shard_map(
        functools.partial(on_device, mesh, radices),
        mesh=mesh,
        in_specs=in_specs,
        out_specs=(P(None, None, both), P(None, None, both)),
        check_vma=False,
    )
```

```python
import functools

import jax
import jax.numpy as jnp
import numpy as np
from jax import lax
from jax.experimental import pallas as pl
from jax.experimental.pallas import tpu as pltpu
from jax.sharding import PartitionSpec as P

MESH = pl.DeviceIdType.MESH
F32, BF16, I32 = jnp.float32, jnp.bfloat16, jnp.int32

section_decay = -567301805773.0 / 1357537059087.0
section_gain = 5161836677717.0 / 13612068292357.0
time_step = 0.05
metric_scale = (1.0, 1.5, 0.75)
end_weight = 0.1

NB = 512
HALF = 64
RADICES = (4, 2, 4)
CHUNKS = ((0, 32), (32, 64), (96, 56), (152, 24))
PACK_ROWS = 176
PACK_ORDER = (5, 8, 1, 4, 0, 2, 3)


def lobatto_slopes():
    root = np.sqrt(3.0 / 7.0)
    x = np.array([-1.0, -root, 0.0, root, 1.0])
    table = np.zeros((5, 5))
    for r in range(5):
        for c in range(5):
            others = [o for o in range(5) if o != r]
            if r == c:
                table[r, c] = sum(1.0 / (x[r] - x[o]) for o in others)
            else:
                top = np.prod([x[r] - x[o] for o in others])
                low = np.prod([x[c] - x[o] for o in range(5) if o != c])
                table[r, c] = top / (low * (x[r] - x[c]))
    return table


def slope_matrices():
    d, e = lobatto_slopes(), np.eye(5)
    full = [np.kron(np.kron(d, e), e), np.kron(np.kron(e, d), e), np.kron(np.kron(e, e), d)]
    full = np.stack([-time_step * g * m for g, m in zip(metric_scale, full)])
    high = full.astype(BF16)
    return np.stack([high, (full - high.astype(np.float64)).astype(BF16)])


def halves(x):
    high = x.astype(BF16)
    return high, (x - high.astype(F32)).astype(BF16)


def moved(x, table, transposed=False):
    rows = x.shape[0]
    high, low = halves(x)
    both = jnp.concatenate([high, low], axis=0)
    dims = (((1,), (1 if transposed else 0,)), ((), ()))
    out = lax.dot_general(both, table, dims, preferred_element_type=F32)
    return out[:rows] + out[rows:]


def reach_of(left, right):
    return jnp.maximum(jnp.abs(left[5]) + left[6], jnp.abs(right[5]) + right[6])


def face_value(left, right, d, reach, f):
    sides = []
    for q in (left, right):
        flux = q[5] * q[f]
        if f == 0 or f == 4:
            flux = flux + q[6] * q[1 + d]
        elif f == 1 + d:
            flux = flux + q[6] * q[4]
        sides.append(flux)
    return sides[0] - sides[1], reach * (right[f] - left[f])


def face_parts(left, right, d):
    reach = reach_of(left, right)
    return zip(*[face_value(left, right, d, reach, f) for f in range(5)])


def one_hot(row, count):
    k = lax.broadcasted_iota(I32, (count, row.shape[1]), 0).astype(F32)
    return jnp.where(k == row, 1.0, 0.0).astype(BF16)


def turned(x, code, inverse):
    lane = lax.broadcasted_iota(I32, (8, 128), 1)
    n = lane & 31
    row = (n * 13) >> 6
    ok = n < 25
    maps = {4: lambda i, k: (k, i), 1: lambda i, k: (4 - i, k), 2: lambda i, k: (i, 4 - k)}
    result = x
    for value in range(1, 8):
        i, k = row, n - row * 5
        for bit in (4, 1, 2) if inverse else (2, 1, 4):
            if value & bit:
                i, k = maps[bit](i, k)
        index = jnp.where(ok, lane - n + i * 5 + k, lane)
        result = jnp.where(code == value, jnp.take_along_axis(x, index, axis=1), result)
    return result


def kernel(
    radices,
    nblk,
    nspan,
    fields,
    store,
    mean,
    sound,
    slot_hbm,
    slopes_hbm,
    turn_hbm,
    offset_hbm,
    acc,
    fixed,
    held,
    turn,
    offset,
    x,
    old,
    slot,
    slopes,
    table,
    pack,
    recv,
    near,
    swaps,
    hot_columns,
    face,
    grid,
    corr,
    sp_send,
    sp_recv,
    own_packet,
    gathered,
    bundle,
    hops,
    final_out,
    final_in,
    load_sem,
    old_sem,
    circ_send,
    circ_recv,
    span_send,
    span_recv,
    hop_send,
    hop_recv,
    plane_send,
    plane_recv,
    far_sem,
):
    t = lax.axis_index("blk")
    slab = lax.axis_index("span")
    after, before = lax.rem(t + 1, nblk), lax.rem(t + nblk - 1, nblk)
    above, below = lax.rem(slab + 1, nspan), lax.rem(slab + nspan - 1, nspan)

    r0, r1, r2 = radices
    z, y, x_at = lax.rem(t, r0), lax.rem(t // r0, r1), t // (r0 * r1)
    is_first, is_last = z == 0, z == r0 - 1
    inner = jnp.logical_and(z > 0, z < r0 - 1)
    run = [t + (lax.rem(z + step, r0) - z) for step in range(1, r0)]
    across = [jnp.logical_and(z == 0, step == r0 - 1) | jnp.logical_and(z == r0 - 1, step == 1) for step in range(1, r0)]
    plane = []
    for dy in range(r1):
        for dx in range(r2):
            if dy or dx:
                to = z + r0 * lax.rem(y + dy, r1) + r0 * r1 * lax.rem(x_at + dx, r2)
                plane.append((dy, dx, to))

    def place(src):
        return held.at[src] if src < 5 else x.at[src - 5]

    def load(src):
        if src < 5:
            array = fields.at[src]
        else:
            array = mean.at[src - 5] if src < 8 else sound
        return [
            pltpu.make_async_copy(array.at[:, pl.ds(128 * b, 128)], place(src).at[b], load_sem.at[src])
            for b in range(4)
        ]

    def arrived_all(ref, sem):
        pltpu.make_async_copy(ref, ref, sem).wait()

    def loaded(src):
        arrived_all(place(src), load_sem.at[src])

    def cells(src, rows=slice(0, 125)):
        return jnp.concatenate([place(src)[b, rows, :] for b in range(4)], axis=1)

    load_slot = pltpu.make_async_copy(slot_hbm, slot, load_sem.at[9])
    load_slopes = pltpu.make_async_copy(slopes_hbm, slopes, load_sem.at[10])
    load_turn = pltpu.make_async_copy(turn_hbm, turn, load_sem.at[11])
    load_offset = pltpu.make_async_copy(offset_hbm, offset, load_sem.at[12])
    load_slot.start()
    for src in PACK_ORDER[:2]:
        for copy in load(src):
            copy.start()

    barrier = pltpu.get_barrier_semaphore()
    for to in (above, below):
        pl.semaphore_signal(barrier, inc=1, device_id={"span": to}, device_id_type=MESH)
    for to, skip in zip(run, across):

        @pl.when(jnp.logical_not(skip))
        def _():
            pl.semaphore_signal(barrier, inc=1, device_id={"blk": to}, device_id_type=MESH)

    @pl.when(inner)
    def _():
        for _, _, to in plane:
            pl.semaphore_signal(barrier, inc=1, device_id={"blk": to}, device_id_type=MESH)

    @pl.when(is_first)
    def _():
        pl.semaphore_signal(barrier, inc=1, device_id={"blk": before}, device_id_type=MESH)

    for src in PACK_ORDER[2:] + (7, 6):
        for copy in load(src):
            copy.start()
    load_slopes.start()
    for f in range(5):
        for b in range(4):
            pltpu.make_async_copy(
                store.at[f, :, pl.ds(128 * b, 128)], old.at[f, b], old_sem.at[0]
            ).start()
    load_turn.start()
    load_offset.start()

    load_slot.wait()
    slot_row = slot[...].astype(F32)
    for end in range(2):
        pack[end, 0:1, :] = slot_row

    def circ(end, part):
        start, rows = CHUNKS[part]
        return pltpu.make_async_remote_copy(
            src_ref=pack.at[end, pl.ds(start, rows), :],
            dst_ref=recv.at[1 - end, pl.ds(start, rows), :],
            send_sem=circ_send.at[end],
            recv_sem=circ_recv.at[1 - end, part],
            device_id={"blk": after if end == 1 else before},
            device_id_type=MESH,
        )

    def start_circ(*parts):
        for part in parts:

            @pl.when(jnp.logical_not(is_last))
            def _():
                circ(1, part).start()

            @pl.when(jnp.logical_not(is_first))
            def _():
                circ(0, part).start()

    every = range(len(CHUNKS))

    def far_start(*parts):
        @pl.when(is_last)
        def _():
            if parts[0] == 0:
                pl.semaphore_wait(barrier, r0 + 1)
                pl.semaphore_signal(far_sem, inc=1, device_id={"blk": after}, device_id_type=MESH)
            for part in parts:
                circ(1, part).start()

    def pack_high(at):
        pack[1, 1 + 25 * at : 26 + 25 * at, :] = cells(PACK_ORDER[at], slice(100, 125))

    loaded(5)
    pack_high(0)
    loaded(8)
    pack_high(1)
    far_start(0)
    loaded(1)
    pack_high(2)
    loaded(4)
    pack_high(3)
    far_start(1)

    lane = lax.broadcasted_iota(I32, (8, NB), 1)
    sub = lax.broadcasted_iota(I32, (8, NB), 0)
    wanted = jnp.where(sub < 4, sub * 128 + (HALF - 1), (sub - 4) * 128 + HALF)
    column = jnp.sum(jnp.where(lane == wanted, slot_row, 0.0), axis=1, keepdims=True)
    hot = jnp.where(lane.astype(F32) == column, 1.0, 0.0)
    wide = jnp.concatenate([hot, jnp.zeros((120, NB), F32)], axis=0)
    hot_columns[...] = jnp.transpose(wide).astype(BF16)

    for src in PACK_ORDER[4:] + (7,):
        loaded(src)
    def pack_faces(d):
        for at, src in enumerate((0, 1, 2, 3, 4, 4 + 1 + d, 8)):
            for end in range(2):
                kind = 2 * (d - 1) + end
                if d == 2:
                    face[kind, 32 * at : 32 * at + 25, :] = cells(src, pl.ds(4 * end, 25, stride=5))
                else:
                    for i in range(5):
                        rows = slice(25 * i + 20 * end, 25 * i + 20 * end + 5)
                        face[kind, 32 * at + 5 * i : 32 * at + 5 * i + 5, :] = cells(src, rows)

    pack_faces(2)
    dims = (((1,), (1,)), ((), ()))
    picked = []
    for kind in (3, 2):
        both = jnp.concatenate(halves(face[kind]), axis=0)
        part = jnp.dot(both, hot_columns[...], preferred_element_type=F32)
        picked.append(part[:256] + part[256:])
    stator_lane = lax.broadcasted_iota(I32, (256, 128), 1) < 4
    packet = jnp.transpose(jnp.where(stator_lane, picked[0], picked[1]))[:8]

    sub1 = lax.broadcasted_iota(I32, (8, 128), 0)
    row = sub1 & 3
    is_stator = sub1 < 4

    def per_row(values):
        out = jnp.full((8, 128), values[3], I32)
        for s in range(3):
            out = jnp.where(row == s, values[s], out)
        return out

    load_turn.wait()
    load_offset.wait()
    code = per_row([turn[0, s] for s in range(4)])
    shift = per_row([offset[s] for s in range(4)])
    shift = jnp.where(is_stator, shift, (nblk - shift) & (nblk - 1))
    own_pair = [packet[:, :128], packet[:, 128:]]
    pair = [jnp.where(is_stator, p, turned(p, code, True)) for p in own_pair]

    for h in range(2):
        own_packet[:, 128 * h : 128 * h + 128] = pair[h]

    def collect(to_z, from_z):
        return pltpu.make_async_remote_copy(
            src_ref=own_packet,
            dst_ref=gathered.at[from_z],
            send_sem=hop_send.at[to_z],
            recv_sem=hop_recv.at[0],
            device_id={"blk": t + to_z - z},
            device_id_type=MESH,
        )

    @pl.when(jnp.logical_not(is_last))
    def _():
        pl.semaphore_wait(barrier, jnp.where(inner, 2 + r0 - 1 + len(plane), r0))

    for to_z in range(1, r0 - 1):

        @pl.when(z != to_z)
        def _():
            collect(to_z, z).start()

    for at in (4, 5, 6):
        pack_high(at)
    far_start(2, 3)
    for at, src in enumerate(PACK_ORDER):
        pack[0, 1 + 25 * at : 26 + 25 * at, :] = cells(src, slice(0, 25))
    start_circ(*every)

    table[...] = one_hot(slot_row, NB)
    loaded(6)
    pack_faces(1)

    def take_collected():
        @pl.when(inner)
        def _():
            arrived_all(gathered.at[pl.ds(0, r0 - 1)], hop_recv.at[0])

        for to_z in range(1, r0 - 1):

            @pl.when(z != to_z)
            def _():
                collect(to_z, 0).wait_send()

        for h in range(2):
            lanes = slice(128 * h, 128 * h + 128)
            for half, target in enumerate((z, outer_z)):
                source = lax.rem(target + r0 - shift0, r0)
                value = pair[h]
                for from_z in range(r0):
                    value = jnp.where((source == from_z) & (z != from_z), gathered[from_z, :, lanes], value)
                bundle[8 * half : 8 * half + 8, lanes] = value

    outer_z = jnp.where(z == 1, 0, r0 - 1)
    shift0 = lax.rem(shift, r0)
    shift1 = lax.rem(shift // r0, r1)
    shift2 = shift // (r0 * r1)

    def hop(number):
        return pltpu.make_async_remote_copy(
            src_ref=bundle,
            dst_ref=hops.at[number],
            send_sem=plane_send.at[0],
            recv_sem=plane_recv.at[0],
            device_id={"blk": plane[number][2]},
            device_id_type=MESH,
        )

    def start_plane():
        @pl.when(inner)
        def _():
            for number in range(len(plane)):
                hop(number).start()

    def take_plane():
        @pl.when(inner)
        def _():
            arrived_all(hops, plane_send.at[0])
            arrived_all(hops, plane_recv.at[0])

        for half, target in enumerate((z, outer_z)):
            up1 = shift1 + jnp.where(target < shift0, 1, 0)
            source1 = lax.rem(y + 2 * r1 - up1, r1)
            move1 = lax.rem(up1, r1)
            move2 = lax.rem(shift2 + (source1 + up1) // r1, r2)
            for h in range(2):
                lanes = slice(128 * h, 128 * h + 128)
                rows = slice(8 * half, 8 * half + 8)
                value = bundle[rows, lanes]
                for number, (dy, dx, _) in enumerate(plane):
                    value = jnp.where((move1 == dy) & (move2 == dx), hops[number, rows, lanes], value)
                final_out[half, :, lanes] = value

    def deliver():
        return pltpu.make_async_remote_copy(
            src_ref=final_out.at[1],
            dst_ref=final_in,
            send_sem=hop_send.at[0],
            recv_sem=hop_send.at[r0 - 1],
            device_id={"blk": lax.rem(t + jnp.where(z == 1, nblk - 1, 1), nblk)},
            device_id_type=MESH,
        )

    for kind in (1, 0):
        grid[kind] = moved(face[kind], table[...])
        for f in range(7):
            sp_send[kind, 25 * f : 25 * f + 25, :] = grid[
                kind, 32 * f : 32 * f + 25, 384 * kind : 384 * kind + 128
            ]


    def span(end):
        return pltpu.make_async_remote_copy(
            src_ref=sp_send.at[end],
            dst_ref=sp_recv.at[1 - end, pl.ds(0, PACK_ROWS), :],
            send_sem=span_send.at[end],
            recv_sem=span_recv.at[1 - end],
            device_id={"span": above if end == 1 else below},
            device_id_type=MESH,
        )

    has_below, has_above = slab > 0, slab < nspan - 1

    def start_span(when):
        @pl.when(jnp.logical_and(when, has_above))
        def _():
            span(1).start()

        @pl.when(jnp.logical_and(when, has_below))
        def _():
            span(0).start()

    start_span(jnp.logical_not(is_last))

    for kind in (2, 3):
        grid[kind] = moved(face[kind], table[...])

    def span_sent():
        @pl.when(has_above)
        def _():
            span(1).wait_send()

        @pl.when(has_below)
        def _():
            span(0).wait_send()

    load_slopes.wait()
    velocity = (5, 6, 7)

    arrived_all(old, old_sem.at[0])

    def volume(f):
        total = None
        for d in range(3):
            fx = cells(velocity[d]) * cells(f)
            if f == 0 or f == 4:
                fx = fx + cells(8) * cells(1 + d)
            elif f == 1 + d:
                fx = fx + cells(8) * cells(4)
            high, low = halves(fx)
            for m, v in ((0, high), (0, low), (1, high)):
                part = jnp.dot(slopes[m, d], v, preferred_element_type=F32)
                total = part if total is None else total + part
        for b in range(4):
            acc[f, b] = section_decay * old[f, b] + total[:, 128 * b : 128 * b + 128]

    volume(0)
    volume(1)
    @pl.when(is_first)
    def _():
        span_sent()
        pl.semaphore_wait(far_sem, 1)
        for part in every:
            circ(0, part).start()

    take_collected()
    start_plane()

    for f in (2, 3, 4):
        volume(f)

    w = 0.5 * time_step * metric_scale[2] / end_weight
    axial = lax.broadcasted_iota(I32, (32, 128), 1)
    for s in range(4):
        cols = slice(128 * s, 128 * s + 128)
        low = [grid[2, 32 * f : 32 * f + 32, cols] for f in range(7)]
        high = [grid[3, 32 * f : 32 * f + 32, cols] for f in range(7)]
        for end in range(2):
            own, far = (high, low) if end else (low, high)
            outer = []
            for f in range(7):
                v = pltpu.roll(far[f], 127 if end else 1, axis=1)
                edge = own[f] if f >= 5 else 0.0
                outer.append(jnp.where(axial == (127 if end else 0), edge, v))
            diff, jump = face_parts(own if end else outer, outer if end else own, 2)
            slides = axial == (HALF - 1 if end else HALF)
            for f in range(5):
                value = diff[f] + jump[f] if end else diff[f] - jump[f]
                corr[2 + end, 32 * f : 32 * f + 32, cols] = jnp.where(slides, 0.0, w * value)

    def add_axial(end, values):
        for f in range(5):
            lines = pl.ds(4 * end, 25, stride=5)
            for b in range(4):
                part = values[32 * f : 32 * f + 25, 128 * b : 128 * b + 128]
                acc[f, b, lines, :] = acc[f, b, lines, :] + part

    for end in range(2):
        add_axial(end, moved(corr[2 + end], table[...], transposed=True))

    far_end = jnp.where(is_last, 1, 0)
    near_end = 1 - far_end
    weight0 = 0.5 * time_step * metric_scale[0] / end_weight

    def settle_rows(end, parts):
        start, stop = CHUNKS[parts[0]][0], sum(CHUNKS[parts[-1]])
        for part in parts:
            first, rows = CHUNKS[part]
            arrived_all(recv.at[end, pl.ds(first, rows), :], circ_recv.at[end, part])
            if part == 0:
                other = one_hot(recv[end, 0:1, :], NB)
                swap = lax.dot_general(other, table[...], dims, preferred_element_type=F32)
                swaps[end] = swap.astype(BF16)
        near[end, start:stop, :] = moved(recv[end, start:stop, :], swaps[end])

    def settle(end, fields, reach=None):
        def side(ref, src):
            at = PACK_ORDER.index(src)
            return ref[end, 1 + 25 * at : 26 + 25 * at, :]

        order = (0, 1, 2, 3, 4, 5, 8)
        own = [side(pack, src) for src in order]
        other = [side(near, src) if src != 3 or 3 in fields else None for src in order]
        if reach is None:
            reach = reach_of(own, other)
        sign = jnp.where(end == 0, weight0, -weight0)
        for f in fields:
            diff, jump = face_value(other, own, 0, reach, f)
            fixed[end, f, 0:25, :] = sign * diff - weight0 * jump
        return reach

    @pl.when(is_last)
    def _():
        arrived_all(pack.at[1], circ_send.at[1])

    start_span(is_last)
    @pl.when(has_above)
    def _():
        span(0).wait_recv()

    @pl.when(has_below)
    def _():
        span(1).wait_recv()

    w = 0.5 * time_step * metric_scale[1] / end_weight
    for b in range(5):
        left, right = [], []
        for f in range(7):
            rows = slice(32 * f, 32 * f + 32)
            if b > 0:
                left.append(grid[1, rows, 128 * b - 128 : 128 * b])
            if b < 4:
                right.append(grid[0, rows, 128 * b : 128 * b + 128])
        for f in range(7):
            rows = slice(32 * f, 32 * f + 32)
            if b == 0:
                wall = -right[f] if f == 2 else right[f]
                left.append(jnp.where(has_below, sp_recv[0, 25 * f : 25 * f + 32, :], wall))
            if b == 4:
                wall = -left[f] if f == 2 else left[f]
                right.append(jnp.where(has_above, sp_recv[1, 25 * f : 25 * f + 32, :], wall))
        diff, jump = face_parts(left, right, 1)
        for f in range(5):
            if b > 0:
                corr[1, 32 * f : 32 * f + 32, 128 * b - 128 : 128 * b] = w * (diff[f] + jump[f])
            if b < 4:
                corr[0, 32 * f : 32 * f + 32, 128 * b : 128 * b + 128] = w * (diff[f] - jump[f])

    for end in range(2):
        back = moved(corr[end], table[...], transposed=True)
        for f in range(5):
            for i in range(5):
                rows = slice(25 * i + 20 * end, 25 * i + 20 * end + 5)
                for b in range(4):
                    part = back[32 * f + 5 * i : 32 * f + 5 * i + 5, 128 * b : 128 * b + 128]
                    acc[f, b, rows, :] += part
    take_plane()

    @pl.when(inner)
    def _():
        deliver().start()

    settle_rows(near_end, (0, 1, 2, 3))
    settle(near_end, (0, 1, 2, 3, 4))
    settle_rows(far_end, (0, 1))
    def slide():
        @pl.when(jnp.logical_not(inner))
        def _():
            deliver().wait_recv()

        pair = []
        for h in range(2):
            lanes = slice(128 * h, 128 * h + 128)
            pair.append(jnp.where(inner, final_out[0, :, lanes], final_in[:, lanes]))
        pair = [jnp.where(is_stator, turned(p, code, False), p) for p in pair]
        outer = [pltpu.roll(p, 4, axis=0) for p in pair]
        left = [jnp.where(is_stator, a, b) for a, b in zip(own_pair, outer)]
        right = [jnp.where(is_stator, b, a) for a, b in zip(own_pair, outer)]

        def values(pair):
            return [pair[f // 4][:, 32 * (f % 4) : 32 * (f % 4) + 32] for f in range(7)]

        w = 0.5 * time_step * metric_scale[2] / end_weight
        diff, jump = face_parts(values(left), values(right), 2)
        sign = jnp.where(is_stator[:, :32], w, -w)
        fixes = jnp.concatenate([w * d + sign * j for d, j in zip(diff, jump)], axis=1)
        fixes = jnp.concatenate(halves(fixes), axis=0)
        tn = (((0,), (0,)), ((), ()))
        spots = jnp.concatenate([jnp.where(sub >= 4, hot, 0.0), jnp.where(sub < 4, hot, 0.0)], axis=1)
        spots = jnp.concatenate([spots, spots], axis=0).astype(BF16)
        spread = lax.dot_general(fixes, spots, tn, preferred_element_type=F32)
        for end in range(2):
            add_axial(end, spread[:, NB * end : NB * end + NB])

    second = lax.rem(slab, 2) == 1
    pl.when(second)(slide)
    settle_rows(far_end, (2,))
    reach = settle(far_end, (0, 1, 2, 4))
    pl.when(jnp.logical_not(second))(slide)
    settle_rows(far_end, (3,))
    settle(far_end, (3,), reach)
    @pl.when(jnp.logical_not(is_first))
    def _():
        span_sent()

    arrived_all(pack.at[0], circ_send.at[0])

    @pl.when(jnp.logical_not(is_last))
    def _():
        arrived_all(pack.at[1], circ_send.at[1])


    @pl.when(inner)
    def _():
        deliver().wait_send()


def update(partial_store, end_parts, fields, fields_next, store_next, ready, sent):
    copies = []
    for f in range(5):
        for b in range(4):
            cols = slice(128 * b, 128 * b + 128)
            for start, stop, end in ((0, 25, 0), (25, 100, None), (100, 125, 1)):
                rows = slice(start, stop)
                value = partial_store[f, b, rows, :]
                if end is not None:
                    value = value + end_parts[end, f, 0:25, cols]
                ready[1, f, rows, cols] = value
                ready[0, f, rows, cols] = fields[f, b, rows, :] + section_gain * value
        for which, result in ((1, store_next), (0, fields_next)):
            copies.append(pltpu.make_async_copy(ready.at[which, f], result.at[f], sent.at[which, f]))
            copies[-1].start()
    for copy in copies:
        copy.wait()


def on_device(mesh, radices, fields, section_store, mean_velocity, sound_speed, element_slot, face_turn, rotor_offset):
    nblk, nspan = mesh.shape["blk"], mesh.shape["span"]
    r0, r1, r2 = radices
    anywhere = pl.BlockSpec(memory_space=pltpu.HBM)
    vmem = pl.BlockSpec(memory_space=pltpu.VMEM)
    dma = pltpu.SemaphoreType.DMA
    partial_store, end_parts, held_fields = pl.pallas_call(
        functools.partial(kernel, radices, nblk, nspan),
        out_shape=(
            jax.ShapeDtypeStruct((5, 4, 125, 128), F32),
            jax.ShapeDtypeStruct((2, 5, 32, NB), F32),
            jax.ShapeDtypeStruct((5, 4, 125, 128), F32),
        ),
        in_specs=[anywhere] * 8,
        out_specs=(vmem, vmem, vmem),
        scratch_shapes=[
            pltpu.SMEM((1, 4), I32),
            pltpu.SMEM((4,), I32),
            pltpu.VMEM((4, 4, 125, 128), F32),
            pltpu.VMEM((5, 4, 125, 128), F32),
            pltpu.VMEM((1, NB), I32),
            pltpu.VMEM((2, 3, 125, 125), BF16),
            pltpu.VMEM((NB, NB), BF16),
            pltpu.VMEM((2, PACK_ROWS, NB), F32),
            pltpu.VMEM((2, PACK_ROWS, NB), F32),
            pltpu.VMEM((2, PACK_ROWS, NB), F32),
            pltpu.VMEM((2, NB, NB), BF16),
            pltpu.VMEM((NB, 128), BF16),
            pltpu.VMEM((4, 256, NB), F32),
            pltpu.VMEM((4, 256, NB), F32),
            pltpu.VMEM((4, 160, NB), F32),
            pltpu.VMEM((2, PACK_ROWS, 128), F32),
            pltpu.VMEM((2, 184, 128), F32),
            pltpu.VMEM((8, 256), F32),
            pltpu.VMEM((r0, 8, 256), F32),
            pltpu.VMEM((16, 256), F32),
            pltpu.VMEM((r1 * r2 - 1, 16, 256), F32),
            pltpu.VMEM((2, 8, 256), F32),
            pltpu.VMEM((8, 256), F32),
            dma((13,)),
            dma((1,)),
            dma((2,)),
            dma((2, len(CHUNKS))),
            dma((2,)),
            dma((2,)),
            dma((r0,)),
            dma((1,)),
            dma((1,)),
            dma((1,)),
            pltpu.SemaphoreType.REGULAR,
        ],
        compiler_params=pltpu.CompilerParams(
            collective_id=0, has_side_effects=True, vmem_limit_bytes=22 * 2**20
        ),
        name="rates",
    )(
        *[
            pltpu.with_memory_space_constraint(value, pltpu.HBM)
            for value in (
                fields,
                section_store,
                mean_velocity,
                sound_speed,
                element_slot.reshape(1, NB),
                jnp.asarray(slope_matrices()),
                face_turn,
                rotor_offset,
            )
        ]
    )
    whole = jax.ShapeDtypeStruct((5, 125, NB), F32)
    fields_next, store_next = pl.pallas_call(
        update,
        out_shape=(whole, whole),
        in_specs=[vmem] * 3,
        out_specs=(anywhere, anywhere),
        scratch_shapes=[
            pltpu.VMEM((2, 5, 125, NB), F32),
            dma((2, 5)),
        ],
        compiler_params=pltpu.CompilerParams(vmem_limit_bytes=12 * 2**20),
        name="update",
    )(partial_store, end_parts, held_fields)
    return fields_next, store_next


def solution(mesh, radices=RADICES):
    both = ("blk", "span")
    in_specs = (
        P(None, None, both),
        P(None, None, both),
        P(None, None, both),
        P(None, both),
        P(both),
        P("blk", "span"),
        P("span"),
    )
    return jax.shard_map(
        functools.partial(on_device, mesh, radices),
        mesh=mesh,
        in_specs=in_specs,
        out_specs=(P(None, None, both), P(None, None, both)),
        check_vma=False,
    )
```
